256 devices in a mesh: seq: 32 (over y, z), head: 8 (over x, core).
Axes of the slice: x: 4, y: 4, z: 8, core: 2. Of those that a mesh axis runs over, the one named last changes fastest.
Arguments:
- query_rows: bfloat16 [32768, 4096], P('seq', 'head'), may hold values from -6 to 6
- key_rows: bfloat16 [32768, 4096], P('seq', 'head'), may hold values from -6 to 6
- value_rows: bfloat16 [32768, 4096], P('seq', 'head'), may hold values from -15 to 15
- block_picks: int32 [64, 32, 4], P('seq', 'head'), may hold values from -1 to 63, as said below
- out_weight: bfloat16 [4096, 4096], P(None, 'head'), may hold values from -0.09375 to 0.09375
Outputs:
- mixed: bfloat16 [32768, 4096], P('seq', 'head')
The draws below stay inside these ranges and needn't reach their ends.
Inputs may be any that keep to these rules, and one draw needn't show every extreme that they name: `block_picks`: every entry that is not -1 names a block held by a lower index of seq than block b. Repeated entries of one row count once. Over the query blocks of one index of seq and the heads of one index of head, at most 2 entries name blocks of any one other index of seq, and every index of seq from 1 on has exactly 2 entries naming blocks of index 0.
All inputs are finite; a program needn't handle non-finite values.
Results may differ from the reference program's by a relative error of at most 0.0059.
Values may be sent and summed in bfloat16 or wider, within the bound.
A program may use at most 192 MiB of HBM per device.

```python
import jax
import jax.numpy as jnp
import numpy as np
from jax import lax

HEADS = 32
HEAD_DIM = 128
D = 4096
BLOCK = 512
TOPK = 5
CAP = 2
BLK_DEV = 2
SEQ = 32768
N_SEQ = 32
N_HEAD = 8


def drawn_pair(key):
    row_count = BLK_DEV * BLOCK * N_SEQ
    width_all = HEADS * HEAD_DIM
    streams = jax.random.split(jax.random.fold_in(key, 7001), 2)
    queries = jnp.clip(1.5 * jax.random.normal(streams[0], (row_count, width_all), jnp.float32), -6.0, 6.0)
    keys_drawn = jnp.clip(1.5 * jax.random.normal(streams[1], (row_count, width_all), jnp.float32), -6.0, 6.0)
    return (queries, keys_drawn)


def draw_query_rows(key, part):
    return drawn_pair(key)[0].astype(jnp.bfloat16)


def draw_key_rows(key, part):
    return drawn_pair(key)[1].astype(jnp.bfloat16)


def draw_block_picks(key, part):
    group_heads = HEADS // N_HEAD
    pair_count = BLK_DEV * group_heads
    slot_count = TOPK - 1
    entry_count = pair_count * slot_count
    seat_count = (N_SEQ - 1) * CAP
    later_count = entry_count - CAP
    later_entries = jnp.asarray(np.array([index_value for index_value in range(entry_count) if index_value % slot_count != 0], dtype=np.int32))

    def one_list(group_id, requester):
        list_key = jax.random.fold_in(jax.random.fold_in(key, 9103), group_id * N_SEQ + requester)
        streams = jax.random.split(list_key, 4)
        first_entries = jax.random.permutation(streams[0], pair_count).astype(jnp.int32) * slot_count
        later_order = jax.random.permutation(streams[1], later_entries).astype(jnp.int32)
        order_list = jnp.concatenate([first_entries, later_order])
        seat_perm = jax.random.permutation(streams[2], seat_count).astype(jnp.int32)
        seat_owner = seat_perm // CAP + 1
        blocked = (seat_owner >= requester).astype(jnp.int32)
        ranked = jnp.argsort(blocked * seat_count + jnp.arange(seat_count, dtype=jnp.int32))
        usable_count = jnp.sum(1 - blocked)
        sorted_owner = jnp.concatenate([seat_owner[ranked], jnp.full((later_count,), -1, jnp.int32)])
        position = jnp.arange(later_count, dtype=jnp.int32)
        later_owner = jnp.where(position < usable_count, sorted_owner[position], -1)
        hot_owner = jnp.where(requester >= 1, jnp.zeros((CAP,), jnp.int32), -1)
        owners = jnp.concatenate([hot_owner, later_owner])
        within = jax.random.randint(streams[3], (entry_count,), 0, BLK_DEV).astype(jnp.int32)
        chosen = jnp.where(owners >= 0, owners * BLK_DEV + within, -1)
        listed = jnp.zeros((entry_count,), jnp.int32).at[order_list].set(chosen)
        return listed.reshape(BLK_DEV, group_heads, slot_count)
    requesters = jnp.arange(N_SEQ, dtype=jnp.int32)
    all_lists = jax.vmap(lambda group_id: jax.vmap(lambda requester: one_list(group_id, requester))(requesters))(jnp.arange(N_HEAD, dtype=jnp.int32))
    all_lists = jnp.transpose(all_lists, (1, 2, 0, 3, 4))
    return all_lists.reshape(N_SEQ * BLK_DEV, HEADS, slot_count)


def block_scale(stream_key, extent, pieces, smallest, high):
    def one(axis_at, shards_of):
        draws = jax.random.uniform(jax.random.fold_in(jax.random.fold_in(stream_key, 6), axis_at), (shards_of,), jnp.float32, smallest / len(pieces), high / len(pieces))
        return jnp.repeat(jnp.exp(draws), extent[axis_at] // shards_of).reshape((-1,) + (1,) * (len(extent) - axis_at - 1))

    factor_of = one(*pieces[0])
    for cut in pieces[1:]:
        factor_of = factor_of * one(*cut)
    return factor_of


def gaussian(rng, dims, deviation, bound, shards=(), held_as=jnp.bfloat16):
    drawn = deviation * jax.random.normal(rng, dims, jnp.float32)
    if shards:
        drawn = drawn * block_scale(rng, dims, shards, -0.22, 0.18)
    return jnp.clip(drawn, -bound, bound).astype(held_as)


def setup_inputs(seed: int = 0) -> dict:
    key_of = jax.random.split(jax.random.key(seed), 6)
    query_rows = draw_query_rows(jax.random.fold_in(key_of[5], 71), 0)
    key_rows = draw_key_rows(jax.random.fold_in(key_of[5], 71), 0)
    value_rows = gaussian(key_of[2], (SEQ, HEADS * HEAD_DIM), 3.0, 15.0, ((0, 32), (1, 8)))
    block_picks = draw_block_picks(jax.random.fold_in(key_of[5], 71), 0)
    out_weight = gaussian(key_of[4], (HEADS * HEAD_DIM, D), (HEADS * HEAD_DIM) ** -0.5, 0.09375, ((1, 8),))
    return {"query_rows": query_rows, "key_rows": key_rows, "value_rows": value_rows, "block_picks": block_picks, "out_weight": out_weight}


def block_partial(query_tile, key_tile, value_tile, causal_mask):
    score_scale = HEAD_DIM ** -0.5
    scores = jnp.einsum("hqd,hkd->hqk", query_tile.astype(jnp.float32), key_tile.astype(jnp.float32)) * score_scale
    if causal_mask is not None:
        scores = jnp.where(causal_mask, scores, -jnp.inf)
    maxima = jnp.max(scores, axis=-1)
    shifted = jnp.exp(scores - maxima[..., None])
    totals = jnp.sum(shifted, axis=-1)
    weights = shifted.astype(jnp.bfloat16)
    partial_out = jnp.einsum("hqk,hkd->hqd", weights.astype(jnp.float32), value_tile.astype(jnp.float32))
    return partial_out.astype(jnp.bfloat16), maxima, totals


def merge_parts(outputs, maxima, totals, usable):
    keep = usable[:, :, None]
    largest = jnp.max(jnp.where(keep, maxima, -jnp.inf), axis=0)
    factor = jnp.where(keep, jnp.exp(maxima - largest[None]), 0.0)
    numer = jnp.sum(factor[..., None] * outputs.astype(jnp.float32), axis=0)
    denom = jnp.sum(factor * totals, axis=0)
    return (numer / denom[..., None]).astype(jnp.bfloat16)


def reference(query_rows, key_rows, value_rows, block_picks, out_weight):
    block_count = query_rows.shape[0] // BLOCK
    block_shape = (block_count, BLOCK, HEADS, HEAD_DIM)
    queries = query_rows.reshape(block_shape)
    key_blocks = key_rows.reshape(block_shape)
    value_blocks = value_rows.reshape(block_shape)
    positions = jnp.arange(BLOCK)
    causal_mask = positions[:, None] >= positions[None, :]
    head_index = jnp.arange(HEADS)

    def one_block(block_id):
        query_tile = jnp.transpose(queries[block_id], (1, 0, 2))
        own_part = block_partial(query_tile, jnp.transpose(key_blocks[block_id], (1, 0, 2)),
                                 jnp.transpose(value_blocks[block_id], (1, 0, 2)), causal_mask)
        chosen = block_picks[block_id]
        part_outputs = [own_part[0]]
        part_maxima = [own_part[1]]
        part_totals = [own_part[2]]
        part_usable = [jnp.ones((HEADS,), dtype=jnp.bool_)]
        for column in range(chosen.shape[1]):
            entries = chosen[:, column]
            usable = entries >= 0
            for earlier in range(column):
                usable = usable & (entries != chosen[:, earlier])
            safe_index = jnp.where(usable, entries, 0)
            result_part = block_partial(query_tile, key_blocks[safe_index, :, head_index, :],
                                        value_blocks[safe_index, :, head_index, :], None)
            part_outputs.append(result_part[0])
            part_maxima.append(result_part[1])
            part_totals.append(result_part[2])
            part_usable.append(usable)
        combined = merge_parts(jnp.stack(part_outputs), jnp.stack(part_maxima), jnp.stack(part_totals),
                               jnp.stack(part_usable))
        return jnp.transpose(combined, (1, 0, 2)).reshape(BLOCK, HEADS * HEAD_DIM)

    attended = lax.map(one_block, jnp.arange(block_count, dtype=jnp.int32)).reshape(-1, HEADS * HEAD_DIM)
    return jnp.dot(attended, out_weight, preferred_element_type=jnp.float32).astype(jnp.bfloat16)
```

```python
import functools

import jax
import jax.numpy as jnp
from jax import lax
from jax.experimental import pallas as pl
from jax.experimental.pallas import tpu as pltpu
from jax.sharding import PartitionSpec as P

CAP = 2
RINGS = {32: (4, 8), 8: (2, 4), 4: (2, 2)}
LOG2E = 1.4426950408889634
MESH = pl.DeviceIdType.MESH


def plan_kernel(per_device, picks, asked, slot_of, meta, used, code):
    blocks, heads, columns = picks.shape
    owners = used.shape[0]

    def clear_owner(d, _):
        used[d] = 0
        return 0

    def clear_slot(i, _):
        asked[i] = 0
        code[i] = 0
        return 0

    lax.fori_loop(0, owners, clear_owner, 0)
    lax.fori_loop(0, owners * CAP, clear_slot, 0)

    def one_pair(pair, _):
        b, h = pair // heads, pair % heads
        entries = [picks[b, h, c] for c in range(columns)]
        for c in range(columns):
            fresh = entries[c] >= 0
            for earlier in range(c):
                fresh = fresh & (entries[c] != entries[earlier])
            block = jnp.maximum(entries[c], 0)
            owner = block // per_device
            rank = used[owner]
            slot = owner * CAP + rank
            slot_of[pair * columns + c] = jnp.where(fresh, slot, -1)

            @pl.when(fresh)
            def _():
                used[owner] = rank + 1
                asked[slot] = pair
                code[slot] = block % per_device * heads + h

        return 0

    lax.fori_loop(0, blocks * heads, one_pair, 0)
    lane = lax.broadcasted_iota(jnp.int32, (1, 128), 1)

    def one_owner(d, _):
        meta[d] = jnp.where(lane == 0, code[d * CAP], code[d * CAP + 1])
        return 0

    lax.fori_loop(0, owners, one_owner, 0)


def plan(block_picks, owners):
    blocks, heads, columns = block_picks.shape
    return pl.pallas_call(
        functools.partial(plan_kernel, blocks),
        out_shape=(
            jax.ShapeDtypeStruct((owners * CAP,), jnp.int32),
            jax.ShapeDtypeStruct((blocks * heads * columns,), jnp.int32),
            jax.ShapeDtypeStruct((owners, 1, 128), jnp.int32),
        ),
        in_specs=[pl.BlockSpec(memory_space=pltpu.SMEM)],
        out_specs=(
            pl.BlockSpec(memory_space=pltpu.SMEM),
            pl.BlockSpec(memory_space=pltpu.SMEM),
            pl.BlockSpec(memory_space=pltpu.VMEM),
        ),
        scratch_shapes=[
            pltpu.SMEM((owners,), jnp.int32),
            pltpu.SMEM((owners * CAP,), jnp.int32),
        ],
    )(block_picks)


def tile_partial(query, key, value_t, causal):
    scale = query.shape[-1] ** (-0.5) * LOG2E
    scores = lax.dot_general(
        key, query, (((1,), (1,)), ((), ())), preferred_element_type=jnp.float32
    )
    if causal:
        key_at = lax.broadcasted_iota(jnp.int32, scores.shape, 0)
        query_at = lax.broadcasted_iota(jnp.int32, scores.shape, 1)
        scores = jnp.where(key_at <= query_at, scores, -1e30)
    top = jnp.max(scores, axis=0, keepdims=True)
    shifted = jnp.exp2((scores - top) * scale)
    total = jnp.sum(shifted, axis=0, keepdims=True)
    part = jnp.dot(value_t, shifted.astype(jnp.bfloat16), preferred_element_type=jnp.float32)
    return part.astype(jnp.bfloat16), jnp.concatenate([top * scale, total], axis=0)


def main_kernel(
    rings,
    asked,
    slot_of,
    meta,
    q_ref,
    k_ref,
    v_ref,
    w_hbm,
    out_ref,
    q_tiles,
    k_tiles,
    v_tiles,
    own_part,
    own_stat,
    meta_in,
    meta_sm,
    q_buf,
    part_buf,
    stat_buf,
    gathered,
    total,
    w_ref,
    meta_s,
    meta_r,
    q_s,
    q_r,
    part_s,
    part_r,
    stat_s,
    stat_r,
    local_sem,
    ring_s,
    ring_r,
    mate_s,
    mate_r,
):
    ny, nz = rings
    count = ny * nz
    pairs, rows, width = q_tiles.shape
    heads = q_ref.shape[1] // width
    blocks = pairs // heads
    columns = slot_of.shape[0] // pairs
    groups = gathered.shape[0]
    me = lax.axis_index("seq")
    y, z = me // nz, me % nz
    head_at = lax.axis_index("head")
    mate = head_at + 1 - 2 * (head_at % 2)
    right = (head_at + 2) % groups
    left = (head_at + groups - 2) % groups
    across = (head_at + 4) % groups

    def shift_of(j):
        i = j // ny
        half = (i + 1) // 2
        dz = (nz // 2 + half * (1 - 2 * (i % 2)) + nz) % nz
        return j % ny, dz

    def target(j):
        dy, dz = shift_of(j)
        return (y + dy) % ny * nz + (z + dz) % nz

    def source(j):
        dy, dz = shift_of(j)
        return (y + ny - dy) % ny * nz + (z + nz - dz) % nz

    def each(body):
        def step(j, carry):
            body(j)
            return carry

        lax.fori_loop(0, count, step, 0)

    def meta_copy(d):
        return pltpu.make_async_remote_copy(
            src_ref=meta.at[d], dst_ref=meta_in.at[me], send_sem=meta_s.at[d],
            recv_sem=meta_r.at[me], device_id={"seq": d}, device_id_type=MESH)

    def q_copy(d):
        return pltpu.make_async_remote_copy(
            src_ref=q_buf.at[pl.ds(d * CAP, CAP)], dst_ref=q_buf.at[pl.ds(me * CAP, CAP)],
            send_sem=q_s.at[d], recv_sem=q_r.at[me], device_id={"seq": d}, device_id_type=MESH)

    def part_copy(d):
        return pltpu.make_async_remote_copy(
            src_ref=part_buf.at[pl.ds(d * CAP, CAP)], dst_ref=part_buf.at[pl.ds(me * CAP, CAP)],
            send_sem=part_s.at[d], recv_sem=part_r.at[me], device_id={"seq": d},
            device_id_type=MESH)

    def stat_copy(d):
        return pltpu.make_async_remote_copy(
            src_ref=stat_buf.at[pl.ds(d * CAP, CAP)], dst_ref=stat_buf.at[pl.ds(me * CAP, CAP)],
            send_sem=stat_s.at[d], recv_sem=stat_r.at[me], device_id={"seq": d},
            device_id_type=MESH)

    def arrival(buf, d, sem):
        here = buf.at[pl.ds(d * CAP, CAP)]
        return pltpu.make_async_remote_copy(
            src_ref=here, dst_ref=here, send_sem=sem.at[d], recv_sem=sem.at[d],
            device_id={"seq": d}, device_id_type=MESH)

    meta_in[...] = jnp.zeros_like(meta_in)
    barrier = pltpu.get_barrier_semaphore()

    def greet(j):
        d = target(j)

        @pl.when(d != me)
        def _():
            pl.semaphore_signal(barrier, inc=1, device_id={"seq": d}, device_id_type=MESH)

    each(greet)
    for other in (mate, right, left):
        pl.semaphore_signal(barrier, inc=1, device_id={"head": other}, device_id_type=MESH)

    w_copy = pltpu.make_async_copy(w_hbm, w_ref, local_sem.at[0])
    w_copy.start()
    for b in range(blocks):
        for h in range(heads):
            q_tiles[b * heads + h] = q_ref[b * rows:(b + 1) * rows, h * width:(h + 1) * width]

    def stage(j):
        d = target(j)

        @pl.when(d < me)
        def _():
            for s in range(CAP):
                q_buf[d * CAP + s] = q_tiles[asked[d * CAP + s]]

    each(stage)
    pl.semaphore_wait(barrier, count + 2)

    def send(j):
        d = target(j)

        @pl.when(d < me)
        def _():
            meta_copy(d).start()
            q_copy(d).start()

    each(send)
    for b in range(blocks):
        for h in range(heads):
            p = b * heads + h
            k_tiles[p] = k_ref[b * rows:(b + 1) * rows, h * width:(h + 1) * width]
            v_tiles[p] = v_ref[b * rows:(b + 1) * rows, h * width:(h + 1) * width].T

    def own(p, carry):
        own_part[p], own_stat[p] = tile_partial(q_tiles[p], k_tiles[p], v_tiles[p], True)
        return carry

    lax.fori_loop(0, pairs, own, 0)

    def meta_wait(j):
        d = source(j)

        @pl.when(d > me)
        def _():
            pltpu.make_async_remote_copy(
                src_ref=meta_in.at[d], dst_ref=meta_in.at[d], send_sem=meta_s.at[d],
                recv_sem=meta_r.at[d], device_id={"seq": d}, device_id_type=MESH).wait_recv()

    each(meta_wait)
    meta_copy_in = pltpu.make_async_copy(meta_in, meta_sm, local_sem.at[1])
    meta_copy_in.start()
    meta_copy_in.wait()

    def serve(j):
        d = source(j)

        @pl.when(d > me)
        def _():
            arrival(q_buf, d, q_r).wait_recv()
            for s in range(CAP):
                i = d * CAP + s
                code = meta_sm[d, 0, s]
                part_buf[i], stat_buf[i] = tile_partial(
                    q_buf[i], k_tiles[code], v_tiles[code], False)
            part_copy(d).start()
            stat_copy(d).start()

    each(serve)

    def collect(j):
        d = target(j)

        @pl.when(d < me)
        def _():
            arrival(part_buf, d, part_r).wait_recv()
            arrival(stat_buf, d, stat_r).wait_recv()

    each(collect)

    def merge(p, carry):
        stats = [own_stat[p]]
        used = [None]
        slots = [None]
        for c in range(columns):
            slot = slot_of[p * columns + c]
            used.append(slot >= 0)
            slots.append(jnp.maximum(slot, 0))
            stats.append(stat_buf[slots[-1]])
        tops = [stats[0][:1]] + [
            jnp.where(used[i], stats[i][:1], -1e30) for i in range(1, columns + 1)]
        largest = functools.reduce(jnp.maximum, tops)
        factor = jnp.exp2(tops[0] - largest)
        numer = factor * own_part[p].astype(jnp.float32)
        denom = factor * stats[0][1:]
        for i in range(1, columns + 1):
            factor = jnp.exp2(tops[i] - largest)
            numer += jnp.where(used[i], factor * part_buf[slots[i]].astype(jnp.float32), 0.0)
            denom += jnp.where(used[i], factor * stats[i][1:], 0.0)
        gathered[head_at, p] = (numer / denom).T.astype(jnp.bfloat16)
        return carry

    def unit(g, b):
        return gathered.at[g, pl.ds(b * heads, heads)]

    def hop(g, b, to, k):
        return pltpu.make_async_remote_copy(
            src_ref=unit(g, b), dst_ref=unit(g, b), send_sem=ring_s.at[k],
            recv_sem=ring_r.at[k], device_id={"head": to}, device_id_type=MESH)

    def pass_over(g, b, k):
        return pltpu.make_async_remote_copy(
            src_ref=unit(g, b), dst_ref=unit(g, b), send_sem=mate_s.at[k],
            recv_sem=mate_r.at[k], device_id={"head": mate}, device_id_type=MESH)

    def project(g, b):
        tiles = jnp.concatenate([gathered[g, b * heads + h] for h in range(heads)], axis=1)
        depth = heads * width
        rows_of = pl.ds(b * rows, rows)
        weight = w_ref[pl.ds(pl.multiple_of(g * depth, depth), depth), :]
        total[rows_of, :] += jnp.dot(tiles, weight, preferred_element_type=jnp.float32)

    total[...] = jnp.zeros_like(total)
    sends = []

    def start(copy):
        copy.start()
        sends.append(copy)

    lax.fori_loop(0, heads, merge, 0)
    start(hop(head_at, 0, right, 0))
    start(pass_over(head_at, 0, 0))
    lax.fori_loop(heads, 2 * heads, merge, 0)
    start(hop(head_at, 1, left, 1))
    start(hop(head_at, 1, right, 2))
    start(hop(head_at, 0, left, 3))
    start(pass_over(head_at, 1, 1))
    w_copy.wait()
    project(head_at, 0)
    project(head_at, 1)
    for b in range(2):
        pass_over(mate, b, b).wait_recv()
        project(mate, b)
    plan_in = [
        (left, 0, right, 0, 4),
        (right, 1, left, 1, 5),
        (left, 1, None, 2, None),
        (right, 0, None, 3, None),
        (across, 0, None, 4, None),
        (across, 1, None, 5, None),
    ]
    flip = 1 - 2 * (head_at % 2)
    for n, (g, b, onward, k, k_next) in enumerate(plan_in):
        hop(g, b, right, k).wait_recv()
        if onward is not None:
            start(hop(g, b, onward, k_next))
        start(pass_over(g, b, 2 + n))
        project(g, b)
        pass_over(g + flip, b, 2 + n).wait_recv()
        project(g + flip, b)
    out_ref[...] = total[...].astype(out_ref.dtype)

    def drain(j):
        d = target(j)

        @pl.when(d < me)
        def _():
            meta_copy(d).wait_send()
            q_copy(d).wait_send()

        @pl.when(d > me)
        def _():
            part_copy(d).wait_send()
            stat_copy(d).wait_send()

    each(drain)
    for copy in sends:
        copy.wait_send()


def attend_and_project(asked, slot_of, meta, query_rows, key_rows, value_rows, out_weight, count,
                       groups, heads):
    tok_rows, feature = query_rows.shape
    width = feature // heads
    pairs = slot_of.shape[0] // 4
    rows = tok_rows * heads // pairs
    slots = count * CAP
    vmem = pl.BlockSpec(memory_space=pltpu.VMEM)
    smem = pl.BlockSpec(memory_space=pltpu.SMEM)
    dma = pltpu.SemaphoreType.DMA
    bf16, f32, i32 = jnp.bfloat16, jnp.float32, jnp.int32
    return pl.pallas_call(
        functools.partial(main_kernel, RINGS[count]),
        out_shape=jax.ShapeDtypeStruct((tok_rows, out_weight.shape[1]), bf16),
        in_specs=[smem, smem, vmem, vmem, vmem, vmem, pl.BlockSpec(memory_space=pl.ANY)],
        out_specs=vmem,
        scratch_shapes=[
            pltpu.VMEM((pairs, rows, width), bf16),
            pltpu.VMEM((pairs, rows, width), bf16),
            pltpu.VMEM((pairs, width, rows), bf16),
            pltpu.VMEM((pairs, width, rows), bf16),
            pltpu.VMEM((pairs, 2, rows), f32),
            pltpu.VMEM((count, 1, 128), i32),
            pltpu.SMEM((count, 1, 128), i32),
            pltpu.VMEM((slots, rows, width), bf16),
            pltpu.VMEM((slots, width, rows), bf16),
            pltpu.VMEM((slots, 2, rows), f32),
            pltpu.VMEM((groups, pairs, rows, width), bf16),
            pltpu.VMEM((tok_rows, out_weight.shape[1]), f32),
            pltpu.VMEM(out_weight.shape, bf16),
        ] + [dma((count,)) for _ in range(8)] + [dma((2,)), dma((6,)), dma((6,)), dma((8,)),
                                                 dma((8,))],
        compiler_params=pltpu.CompilerParams(
            collective_id=0, has_side_effects=True, vmem_limit_bytes=60 * 1024 * 1024),
    )(asked, slot_of, meta, query_rows, key_rows, value_rows, out_weight)


def solution(mesh):
    count, groups = mesh.shape["seq"], mesh.shape["head"]

    def body(query_rows, key_rows, value_rows, block_picks, out_weight):
        asked, slot_of, meta = plan(block_picks, count)
        return attend_and_project(asked, slot_of, meta, query_rows, key_rows, value_rows,
                                  out_weight, count, groups, block_picks.shape[1])

    return jax.shard_map(
        body,
        mesh=mesh,
        in_specs=(
            P("seq", "head"),
            P("seq", "head"),
            P("seq", "head"),
            P("seq", "head", None),
            P(None, "head"),
        ),
        out_specs=P("seq", "head"),
        check_vma=False,
    )
```

```python
import functools

import jax
import jax.numpy as jnp
from jax import lax
from jax.experimental import pallas as pl
from jax.experimental.pallas import tpu as pltpu
from jax.sharding import PartitionSpec as P

CAP = 2
RINGS = {32: (4, 8)}
LOG2E = 1.4426950408889634
MESH = pl.DeviceIdType.MESH


def plan_kernel(ring, per_device, picks, slot_of, requests, used):
    blocks, heads, columns = picks.shape
    owners = used.shape[0]
    rows_of_owners = requests.shape[0]

    def clear_owner(d, _):
        used[d] = 0
        return 0

    def clear_request(i, _):
        for row in range(rows_of_owners):
            requests[row, i] = 0
        return 0

    lax.fori_loop(0, owners, clear_owner, 0)
    lax.fori_loop(0, 2 * ring * CAP, clear_request, 0)

    def one_pair(pair, _):
        b, h = pair // heads, pair % heads
        entries = [picks[b, h, c] for c in range(columns)]
        for c in range(columns):
            fresh = entries[c] >= 0
            for earlier in range(c):
                fresh = fresh & (entries[c] != entries[earlier])
            block = jnp.maximum(entries[c], 0)
            owner = block // per_device
            rank = used[owner]
            slot_of[pair * columns + c] = jnp.where(fresh, owner * CAP + rank, -1)

            @pl.when(fresh)
            def _():
                used[owner] = rank + 1
                at = owner % ring * CAP + rank
                requests[owner // ring, at] = block % per_device * heads + h
                requests[owner // ring, ring * CAP + at] = pair

        return 0

    lax.fori_loop(0, blocks * heads, one_pair, 0)


def plan(block_picks, rings):
    blocks, heads, columns = block_picks.shape
    ny, nz = rings
    smem = pl.BlockSpec(memory_space=pltpu.SMEM)
    return pl.pallas_call(
        functools.partial(plan_kernel, nz, blocks),
        out_shape=(
            jax.ShapeDtypeStruct((blocks * heads * columns,), jnp.int32),
            jax.ShapeDtypeStruct((ny, 128), jnp.int32),
        ),
        in_specs=[smem],
        out_specs=(smem, smem),
        scratch_shapes=[pltpu.SMEM((ny * nz,), jnp.int32)],
    )(block_picks)


def tile_partial(query, key, value_t, causal):
    scale = query.shape[-1] ** (-0.5) * LOG2E
    scores = lax.dot_general(
        key, query, (((1,), (1,)), ((), ())), preferred_element_type=jnp.float32
    )
    if causal:
        key_at = lax.broadcasted_iota(jnp.int32, scores.shape, 0)
        query_at = lax.broadcasted_iota(jnp.int32, scores.shape, 1)
        scores = jnp.where(key_at <= query_at, scores, -1e30)
    top = jnp.max(scores, axis=0, keepdims=True)
    shifted = jnp.exp2((scores - top) * scale)
    total = jnp.sum(shifted, axis=0, keepdims=True)
    part = jnp.dot(value_t, shifted.astype(jnp.bfloat16), preferred_element_type=jnp.float32)
    return part.astype(jnp.bfloat16), jnp.concatenate([top * scale, total], axis=0)


def main_kernel(
    rings,
    slot_of,
    requests,
    q_ref,
    k_ref,
    v_ref,
    w_hbm,
    out_ref,
    queries,
    own_part,
    own_stat,
    asks,
    asks_sm,
    part_buf,
    stat_buf,
    gathered,
    total,
    w_ref,
    ask_s,
    ask_r,
    q_s,
    q_r,
    part_s,
    part_r,
    stat_s,
    stat_r,
    key_s,
    key_r,
    value_s,
    value_r,
    local_sem,
    ring_s,
    ring_r,
    mate_s,
    mate_r,
    *chunks,
):
    ny, nz = rings
    _, pairs, rows, width = queries.shape
    heads = q_ref.shape[1] // width
    blocks = pairs // heads
    columns = slot_of.shape[0] // pairs
    groups = gathered.shape[0]
    half = nz // 2
    keys, values_t = chunks[:nz], chunks[nz:]
    held = [[0] + [way * (half - 1) + step for step in range(1, half)] + [nz - 1]
            for way in (0, 1)]
    me = lax.axis_index("seq")
    y, z = me // nz, me % nz
    head_at = lax.axis_index("head")
    mate = head_at + 1 - 2 * (head_at % 2)
    right = (head_at + 2) % groups
    left = (head_at + groups - 2) % groups
    across = (head_at + 4) % groups

    def remote(src, dst, send_sem, recv_sem, to):
        return pltpu.make_async_remote_copy(
            src_ref=src, dst_ref=dst, send_sem=send_sem, recv_sem=recv_sem, device_id=to,
            device_id_type=MESH)

    def along_y(row):
        return {"seq": row * nz + z}

    def ask_copy(row):
        return remote(requests.at[row], asks.at[y], ask_s.at[row], ask_r.at[y], along_y(row))

    def query_copy(row):
        return remote(queries.at[y], queries.at[y], q_s.at[row], q_r.at[y], along_y(row))

    def part_copy(row, at):
        src = part_buf.at[pl.ds((row * nz + at) * CAP, CAP)]
        dst = part_buf.at[pl.ds((y * nz + at) * CAP, CAP)]
        return remote(src, dst, part_s.at[row, at], part_r.at[y, at], along_y(row))

    def stat_copy(row, at):
        src = stat_buf.at[pl.ds((row * nz + at) * CAP, CAP)]
        dst = stat_buf.at[pl.ds((y * nz + at) * CAP, CAP)]
        return remote(src, dst, stat_s.at[row, at], stat_r.at[y, at], along_y(row))

    def ring_copy(bufs, sems, way, step):
        turn = 1 - 2 * way
        to = {"seq": y * nz + (z + nz + turn) % nz}
        return remote(bufs[held[way][step]], bufs[held[way][step + 1]], sems[0].at[way, step],
                      sems[1].at[way, step], to)

    def key_copy(way, step):
        return ring_copy(keys, (key_s, key_r), way, step)

    def value_copy(way, step):
        return ring_copy(values_t, (value_s, value_r), way, step)

    def from_below(body):
        def step(row, carry):
            @pl.when(row < y)
            def _():
                body(row)

            return carry

        lax.fori_loop(0, ny, step, 0)

    def from_above(body):
        def step(row, carry):
            @pl.when(row > y)
            def _():
                body(row)

            return carry

        lax.fori_loop(0, ny, step, 0)

    asks[...] = jnp.zeros_like(asks)
    asks[y] = requests[y]
    barrier = pltpu.get_barrier_semaphore()
    for step in range(1, ny):
        pl.semaphore_signal(barrier, inc=1, device_id=along_y((y + step) % ny),
                            device_id_type=MESH)
    for step in (1, nz - 1):
        pl.semaphore_signal(barrier, inc=1, device_id={"seq": y * nz + (z + step) % nz},
                            device_id_type=MESH)
    for other in (mate, right, left):
        pl.semaphore_signal(barrier, inc=1, device_id={"head": other}, device_id_type=MESH)

    w_copy = pltpu.make_async_copy(w_hbm, w_ref, local_sem.at[0])
    w_copy.start()

    def tile(ref, b, h):
        return ref[b * rows:(b + 1) * rows, h * width:(h + 1) * width]

    for b in range(blocks):
        for h in range(heads):
            keys[0][b * heads + h] = tile(k_ref, b, h)
            queries[y, b * heads + h] = tile(q_ref, b, h)
    pl.semaphore_wait(barrier, ny - 1 + 2 + 3)
    from_below(lambda row: ask_copy(row).start())
    key_copy(0, 0).start()
    key_copy(1, 0).start()
    from_below(lambda row: query_copy(row).start())
    for b in range(blocks):
        for h in range(heads):
            values_t[0][b * heads + h] = tile(v_ref, b, h).T
    value_copy(0, 0).start()
    value_copy(1, 0).start()

    def own(p, carry):
        own_part[p], own_stat[p] = tile_partial(
            queries[y, p], keys[0][p], values_t[0][p], True)
        return carry

    lax.fori_loop(0, pairs, own, 0)
    from_above(lambda row: remote(
        requests.at[row], asks.at[row], ask_s.at[row], ask_r.at[row], along_y(row)).wait_recv())
    ask_copy_in = pltpu.make_async_copy(asks, asks_sm, local_sem.at[1])
    ask_copy_in.start()
    ask_copy_in.wait()

    def serve_row(row, at, n):
        for s in range(CAP):
            code = asks_sm[row, 0, at * CAP + s]
            pair = asks_sm[row, 0, (nz + at) * CAP + s]
            i = (row * nz + at) * CAP + s
            part_buf[i], stat_buf[i] = tile_partial(
                queries[row, pair], keys[n][code], values_t[n][code], False)

    def serve(at, n):
        def one(row, carry):
            @pl.when((row > y) | ((row == y) & (at < z)))
            def _():
                serve_row(row, at, n)

            @pl.when(row > y)
            def _():
                part_copy(row, at).start()
                stat_copy(row, at).start()

            return carry

        lax.fori_loop(0, ny, one, 0)

    for step in range(1, half):
        for copy_of, last_way in ((key_copy, 0), (value_copy, 1)):
            for way in (0, 1):
                copy_of(way, step - 1).wait_recv()
                if step < half - 1 or way == last_way:
                    copy_of(way, step).start()
        if step == 1:
            from_above(lambda row: remote(
                queries.at[row], queries.at[row], q_s.at[row], q_r.at[row],
                along_y(row)).wait_recv())
            serve(z, 0)
        serve((z + nz - step) % nz, held[0][step])
        serve((z + step) % nz, held[1][step])
    key_copy(0, half - 1).wait_recv()
    value_copy(1, half - 1).wait_recv()
    serve((z + half) % nz, nz - 1)

    def collect(row):
        def one(at, carry):
            here = pl.ds((row * nz + at) * CAP, CAP)
            remote(part_buf.at[here], part_buf.at[here], part_s.at[row, at], part_r.at[row, at],
                   along_y(row)).wait_recv()
            remote(stat_buf.at[here], stat_buf.at[here], stat_s.at[row, at], stat_r.at[row, at],
                   along_y(row)).wait_recv()
            return carry

        lax.fori_loop(0, nz, one, 0)

    from_below(collect)

    def merge(p, carry):
        stats = [own_stat[p]]
        used = [None]
        slots = [None]
        for c in range(columns):
            slot = slot_of[p * columns + c]
            used.append(slot >= 0)
            slots.append(jnp.maximum(slot, 0))
            stats.append(stat_buf[slots[-1]])
        tops = [stats[0][:1]] + [
            jnp.where(used[i], stats[i][:1], -1e30) for i in range(1, columns + 1)]
        largest = functools.reduce(jnp.maximum, tops)
        factor = jnp.exp2(tops[0] - largest)
        numer = factor * own_part[p].astype(jnp.float32)
        denom = factor * stats[0][1:]
        for i in range(1, columns + 1):
            factor = jnp.exp2(tops[i] - largest)
            numer += jnp.where(used[i], factor * part_buf[slots[i]].astype(jnp.float32), 0.0)
            denom += jnp.where(used[i], factor * stats[i][1:], 0.0)
        gathered[head_at, p] = (numer / denom).T.astype(jnp.bfloat16)
        return carry

    def unit(g, b):
        return gathered.at[g, pl.ds(b * heads, heads)]

    def hop(g, b, to, k):
        return pltpu.make_async_remote_copy(
            src_ref=unit(g, b), dst_ref=unit(g, b), send_sem=ring_s.at[k],
            recv_sem=ring_r.at[k], device_id={"head": to}, device_id_type=MESH)

    def pass_over(g, b, k):
        return pltpu.make_async_remote_copy(
            src_ref=unit(g, b), dst_ref=unit(g, b), send_sem=mate_s.at[k],
            recv_sem=mate_r.at[k], device_id={"head": mate}, device_id_type=MESH)

    def project(g, b):
        tiles = jnp.concatenate([gathered[g, b * heads + h] for h in range(heads)], axis=1)
        depth = heads * width
        rows_of = pl.ds(b * rows, rows)
        weight = w_ref[pl.ds(pl.multiple_of(g * depth, depth), depth), :]
        total[rows_of, :] += jnp.dot(tiles, weight, preferred_element_type=jnp.float32)

    total[...] = jnp.zeros_like(total)
    sends = []

    def start(copy):
        copy.start()
        sends.append(copy)

    lax.fori_loop(0, heads, merge, 0)
    start(hop(head_at, 0, right, 0))
    start(pass_over(head_at, 0, 0))
    lax.fori_loop(heads, 2 * heads, merge, 0)
    start(hop(head_at, 1, left, 1))
    start(hop(head_at, 1, right, 2))
    start(hop(head_at, 0, left, 3))
    start(pass_over(head_at, 1, 1))
    w_copy.wait()
    project(head_at, 0)
    project(head_at, 1)
    for b in range(2):
        pass_over(mate, b, b).wait_recv()
        project(mate, b)
    plan_in = [
        (left, 0, right, 0, 4),
        (right, 1, left, 1, 5),
        (left, 1, None, 2, None),
        (right, 0, None, 3, None),
        (across, 0, None, 4, None),
        (across, 1, None, 5, None),
    ]
    flip = 1 - 2 * (head_at % 2)
    for n, (g, b, onward, k, k_next) in enumerate(plan_in):
        hop(g, b, right, k).wait_recv()
        if onward is not None:
            start(hop(g, b, onward, k_next))
        start(pass_over(g, b, 2 + n))
        project(g, b)
        pass_over(g + flip, b, 2 + n).wait_recv()
        project(g + flip, b)
    out_ref[...] = total[...].astype(out_ref.dtype)

    def drain_below(row):
        ask_copy(row).wait_send()
        query_copy(row).wait_send()

    def drain_above(row):
        def one(at, carry):
            part_copy(row, at).wait_send()
            stat_copy(row, at).wait_send()
            return carry

        lax.fori_loop(0, nz, one, 0)

    from_below(drain_below)
    from_above(drain_above)
    for way in (0, 1):
        for step in range(half):
            if step < half - 1 or way == 0:
                key_copy(way, step).wait_send()
            if step < half - 1 or way == 1:
                value_copy(way, step).wait_send()
    for copy in sends:
        copy.wait_send()


def attend_and_project(slot_of, requests, query_rows, key_rows, value_rows, out_weight, rings,
                       groups, heads, pairs):
    ny, nz = rings
    tok_rows, feature = query_rows.shape
    width = feature // heads
    rows = tok_rows * heads // pairs
    slots = ny * nz * CAP
    vmem = pl.BlockSpec(memory_space=pltpu.VMEM)
    smem = pl.BlockSpec(memory_space=pltpu.SMEM)
    dma = pltpu.SemaphoreType.DMA
    bf16, f32, i32 = jnp.bfloat16, jnp.float32, jnp.int32
    return pl.pallas_call(
        functools.partial(main_kernel, rings),
        out_shape=jax.ShapeDtypeStruct((tok_rows, out_weight.shape[1]), bf16),
        in_specs=[smem, vmem, vmem, vmem, vmem, pl.BlockSpec(memory_space=pl.ANY)],
        out_specs=vmem,
        scratch_shapes=[
            pltpu.VMEM((ny, pairs, rows, width), bf16),
            pltpu.VMEM((pairs, width, rows), bf16),
            pltpu.VMEM((pairs, 2, rows), f32),
            pltpu.VMEM((ny, 1, 128), i32),
            pltpu.SMEM((ny, 1, 128), i32),
            pltpu.VMEM((slots, width, rows), bf16),
            pltpu.VMEM((slots, 2, rows), f32),
            pltpu.VMEM((groups, pairs, rows, width), bf16),
            pltpu.VMEM((tok_rows, out_weight.shape[1]), f32),
            pltpu.VMEM(out_weight.shape, bf16),
        ]
        + [dma((ny,)) for _ in range(4)]
        + [dma((ny, nz)) for _ in range(4)]
        + [dma((2, nz // 2)) for _ in range(4)]
        + [dma((2,)), dma((6,)), dma((6,)), dma((8,)), dma((8,))]
        + [pltpu.VMEM((pairs, rows, width), bf16) for _ in range(nz)]
        + [pltpu.VMEM((pairs, width, rows), bf16) for _ in range(nz)],
        compiler_params=pltpu.CompilerParams(
            collective_id=0, has_side_effects=True, vmem_limit_bytes=60 * 1024 * 1024),
    )(slot_of, requests, query_rows, key_rows, value_rows, out_weight)


def solution(mesh):
    rings, groups = RINGS[mesh.shape["seq"]], mesh.shape["head"]

    def body(query_rows, key_rows, value_rows, block_picks, out_weight):
        blocks, heads, _ = block_picks.shape
        slot_of, requests = plan(block_picks, rings)
        return attend_and_project(slot_of, requests[:, None], query_rows, key_rows, value_rows,
                                  out_weight, rings, groups, heads, blocks * heads)

    return jax.shard_map(
        body,
        mesh=mesh,
        in_specs=(
            P("seq", "head"),
            P("seq", "head"),
            P("seq", "head"),
            P("seq", "head", None),
            P(None, "head"),
        ),
        out_specs=P("seq", "head"),
        check_vma=False,
    )
```

```python
import functools

import jax
import jax.numpy as jnp
from jax import lax
from jax.experimental import pallas as pl
from jax.experimental.pallas import tpu as pltpu
from jax.sharding import PartitionSpec as P

CAP = 2
RINGS = {32: (4, 8)}
LOG2E = 1.4426950408889634
MESH = pl.DeviceIdType.MESH


def plan_kernel(ring, per_device, picks, slot_of, requests, used):
    blocks, heads, columns = picks.shape
    owners = used.shape[0]
    rows_of_owners = requests.shape[0]

    def clear_owner(d, _):
        used[d] = 0
        return 0

    def clear_request(i, _):
        for row in range(rows_of_owners):
            requests[row, i] = 0
        return 0

    lax.fori_loop(0, owners, clear_owner, 0)
    lax.fori_loop(0, 2 * ring * CAP, clear_request, 0)

    def one_pair(pair, _):
        b, h = pair // heads, pair % heads
        entries = [picks[b, h, c] for c in range(columns)]
        for c in range(columns):
            fresh = entries[c] >= 0
            for earlier in range(c):
                fresh = fresh & (entries[c] != entries[earlier])
            block = jnp.maximum(entries[c], 0)
            owner = block // per_device
            rank = used[owner]
            slot_of[pair * columns + c] = jnp.where(fresh, owner * CAP + rank, -1)

            @pl.when(fresh)
            def _():
                used[owner] = rank + 1
                at = owner % ring * CAP + rank
                requests[owner // ring, at] = block % per_device * heads + h
                requests[owner // ring, ring * CAP + at] = pair

        return 0

    lax.fori_loop(0, blocks * heads, one_pair, 0)


def plan(block_picks, rings):
    blocks, heads, columns = block_picks.shape
    ny, nz = rings
    smem = pl.BlockSpec(memory_space=pltpu.SMEM)
    return pl.pallas_call(
        functools.partial(plan_kernel, nz, blocks),
        out_shape=(
            jax.ShapeDtypeStruct((blocks * heads * columns,), jnp.int32),
            jax.ShapeDtypeStruct((ny, 128), jnp.int32),
        ),
        in_specs=[smem],
        out_specs=(smem, smem),
        scratch_shapes=[pltpu.SMEM((ny * nz,), jnp.int32)],
    )(block_picks)


def tile_partial(query, key, value_t, causal):
    scale = query.shape[-1] ** (-0.5) * LOG2E
    scores = lax.dot_general(
        key, query, (((1,), (1,)), ((), ())), preferred_element_type=jnp.float32
    )
    if causal:
        key_at = lax.broadcasted_iota(jnp.int32, scores.shape, 0)
        query_at = lax.broadcasted_iota(jnp.int32, scores.shape, 1)
        scores = jnp.where(key_at <= query_at, scores, -1e30)
    top = jnp.max(scores, axis=0, keepdims=True)
    shifted = jnp.exp2((scores - top) * scale)
    total = jnp.sum(shifted, axis=0, keepdims=True)
    part = jnp.dot(value_t, shifted.astype(jnp.bfloat16), preferred_element_type=jnp.float32)
    return part.astype(jnp.bfloat16), jnp.concatenate([top * scale, total], axis=0)


def main_kernel(
    rings,
    slot_of,
    requests,
    q_ref,
    k_ref,
    v_ref,
    w_hbm,
    out_ref,
    queries,
    own_part,
    own_stat,
    asks,
    asks_sm,
    part_buf,
    stat_buf,
    gathered,
    total,
    w_ref,
    ask_s,
    ask_r,
    q_s,
    q_r,
    part_s,
    part_r,
    stat_s,
    stat_r,
    key_s,
    key_r,
    value_s,
    value_r,
    local_sem,
    ring_s,
    ring_r,
    mate_s,
    mate_r,
    q_go,
    ring_go,
    *chunks,
):
    ny, nz = rings
    _, pairs, rows, width = queries.shape
    heads = q_ref.shape[1] // width
    blocks = pairs // heads
    columns = slot_of.shape[0] // pairs
    groups = gathered.shape[0]
    half = nz // 2
    keys, values_t = chunks[:nz], chunks[nz:]
    held = [[0] + [way * (half - 1) + step for step in range(1, half)] + [nz - 1]
            for way in (0, 1)]
    me = lax.axis_index("seq")
    y, z = me // nz, me % nz
    head_at = lax.axis_index("head")
    mate = head_at + 1 - 2 * (head_at % 2)
    right = (head_at + 2) % groups
    left = (head_at + groups - 2) % groups
    across = (head_at + 4) % groups
    leads = head_at % 2 == 0
    follows = head_at % 2 == 1

    def remote(src, dst, send_sem, recv_sem, to):
        return pltpu.make_async_remote_copy(
            src_ref=src, dst_ref=dst, send_sem=send_sem, recv_sem=recv_sem, device_id=to,
            device_id_type=MESH)

    def along_y(row):
        return {"seq": row * nz + z}

    def ask_copy(row):
        return remote(requests.at[row], asks.at[y], ask_s.at[row], ask_r.at[y], along_y(row))

    def query_copy(row):
        return remote(queries.at[y], queries.at[y], q_s.at[row], q_r.at[y], along_y(row))

    def part_copy(row, at):
        src = part_buf.at[pl.ds((row * nz + at) * CAP, CAP)]
        dst = part_buf.at[pl.ds((y * nz + at) * CAP, CAP)]
        return remote(src, dst, part_s.at[row, at], part_r.at[y, at], along_y(row))

    def stat_copy(row, at):
        src = stat_buf.at[pl.ds((row * nz + at) * CAP, CAP)]
        dst = stat_buf.at[pl.ds((y * nz + at) * CAP, CAP)]
        return remote(src, dst, stat_s.at[row, at], stat_r.at[y, at], along_y(row))

    def ring_copy(bufs, sems, way, step):
        turn = 1 - 2 * way
        to = {"seq": y * nz + (z + nz + turn) % nz}
        return remote(bufs[held[way][step]], bufs[held[way][step + 1]], sems[0].at[way, step],
                      sems[1].at[way, step], to)

    def key_copy(way, step):
        return ring_copy(keys, (key_s, key_r), way, step)

    def value_copy(way, step):
        return ring_copy(values_t, (value_s, value_r), way, step)

    def from_below(body):
        def step(row, carry):
            @pl.when(row < y)
            def _():
                body(row)

            return carry

        lax.fori_loop(0, ny, step, 0)

    def from_above(body):
        def step(row, carry):
            @pl.when(row > y)
            def _():
                body(row)

            return carry

        lax.fori_loop(0, ny, step, 0)

    asks[...] = jnp.zeros_like(asks)
    asks[y] = requests[y]
    barrier = pltpu.get_barrier_semaphore()
    for step in range(1, ny):
        pl.semaphore_signal(barrier, inc=1, device_id=along_y((y + step) % ny),
                            device_id_type=MESH)
    for step in (1, nz - 1):
        pl.semaphore_signal(barrier, inc=1, device_id={"seq": y * nz + (z + step) % nz},
                            device_id_type=MESH)
    for other in (mate, right, left):
        pl.semaphore_signal(barrier, inc=1, device_id={"head": other}, device_id_type=MESH)

    w_copy = pltpu.make_async_copy(w_hbm, w_ref, local_sem.at[0])
    w_copy.start()

    def tile(ref, b, h):
        return ref[b * rows:(b + 1) * rows, h * width:(h + 1) * width]

    for b in range(blocks):
        for h in range(heads):
            keys[0][b * heads + h] = tile(k_ref, b, h)
            queries[y, b * heads + h] = tile(q_ref, b, h)
    pl.semaphore_wait(barrier, ny - 1 + 2 + 3)
    def start_queries():
        from_below(lambda row: query_copy(row).start())

    def start_ring():
        for way in (0, 1):
            key_copy(way, 0).start()
        for way in (0, 1):
            value_copy(way, 0).start()

    from_below(lambda row: ask_copy(row).start())

    @pl.when(leads)
    def _():
        key_copy(0, 0).start()
        key_copy(1, 0).start()
        start_queries()

    for b in range(blocks):
        for h in range(heads):
            values_t[0][b * heads + h] = tile(v_ref, b, h).T

    @pl.when(leads)
    def _():
        value_copy(0, 0).start()
        value_copy(1, 0).start()

    def own(p, carry):
        own_part[p], own_stat[p] = tile_partial(
            queries[y, p], keys[0][p], values_t[0][p], True)
        return carry

    lax.fori_loop(0, pairs, own, 0)
    total[...] = jnp.zeros_like(total)
    w_copy.wait()

    @pl.when(follows)
    def _():
        pl.semaphore_wait(q_go, 1)
        start_queries()
        pl.semaphore_wait(ring_go, 1)
        start_ring()

    from_above(lambda row: remote(
        requests.at[row], asks.at[row], ask_s.at[row], ask_r.at[row], along_y(row)).wait_recv())
    ask_copy_in = pltpu.make_async_copy(asks, asks_sm, local_sem.at[1])
    ask_copy_in.start()
    ask_copy_in.wait()

    def serve_row(row, at, n):
        for s in range(CAP):
            code = asks_sm[row, 0, at * CAP + s]
            pair = asks_sm[row, 0, (nz + at) * CAP + s]
            i = (row * nz + at) * CAP + s
            part_buf[i], stat_buf[i] = tile_partial(
                queries[row, pair], keys[n][code], values_t[n][code], False)

    def serve(at, n):
        def one(i, carry):
            row = ny - 1 - i

            @pl.when((row > y) | ((row == y) & (at < z)))
            def _():
                serve_row(row, at, n)

            @pl.when(row > y)
            def _():
                part_copy(row, at).start()
                stat_copy(row, at).start()

            return carry

        lax.fori_loop(0, ny, one, 0)

    for step in range(1, half):
        for copy_of, last_way in ((key_copy, 0), (value_copy, 1)):
            for way in (0, 1):
                copy_of(way, step - 1).wait_recv()
                if step < half - 1 or way == last_way:
                    copy_of(way, step).start()
        if step == 1:
            @pl.when(leads)
            def _():
                pl.semaphore_signal(q_go, inc=1, device_id={"head": mate}, device_id_type=MESH)

            from_above(lambda row: remote(
                queries.at[row], queries.at[row], q_s.at[row], q_r.at[row],
                along_y(row)).wait_recv())
            serve(z, 0)
        if step == half - 1:
            @pl.when(leads)
            def _():
                pl.semaphore_signal(ring_go, inc=1, device_id={"head": mate}, device_id_type=MESH)

        serve((z + nz - step) % nz, held[0][step])
        serve((z + step) % nz, held[1][step])
    def unit(g, b):
        return gathered.at[g, pl.ds(b * heads, heads)]

    def hop(g, b, to, k):
        return pltpu.make_async_remote_copy(
            src_ref=unit(g, b), dst_ref=unit(g, b), send_sem=ring_s.at[k],
            recv_sem=ring_r.at[k], device_id={"head": to}, device_id_type=MESH)

    def pass_over(g, b, k):
        return pltpu.make_async_remote_copy(
            src_ref=unit(g, b), dst_ref=unit(g, b), send_sem=mate_s.at[k],
            recv_sem=mate_r.at[k], device_id={"head": mate}, device_id_type=MESH)

    def project(g, b):
        tiles = jnp.concatenate([gathered[g, b * heads + h] for h in range(heads)], axis=1)
        depth = heads * width
        rows_of = pl.ds(b * rows, rows)
        weight = w_ref[pl.ds(pl.multiple_of(g * depth, depth), depth), :]
        total[rows_of, :] += jnp.dot(tiles, weight, preferred_element_type=jnp.float32)

    arrivals = [
        (left, 0, right, 0, 4),
        (right, 1, left, 1, 5),
        (left, 1, None, 2, None),
        (right, 0, None, 3, None),
        (across, 0, None, 4, None),
        (across, 1, None, 5, None),
    ]
    flip = 1 - 2 * (head_at % 2)

    def project_mates():
        for b in range(2):
            pass_over(mate, b, b).wait_recv()
            project(mate, b)
        for n, (g, b, _, _, _) in enumerate(arrivals):
            pass_over(g + flip, b, 2 + n).wait_recv()
            project(g + flip, b)

    pl.when(follows)(project_mates)
    key_copy(0, half - 1).wait_recv()
    value_copy(1, half - 1).wait_recv()
    serve((z + half) % nz, nz - 1)

    def collect(row):
        def one(at, carry):
            here = pl.ds((row * nz + at) * CAP, CAP)
            remote(part_buf.at[here], part_buf.at[here], part_s.at[row, at], part_r.at[row, at],
                   along_y(row)).wait_recv()
            remote(stat_buf.at[here], stat_buf.at[here], stat_s.at[row, at], stat_r.at[row, at],
                   along_y(row)).wait_recv()
            return carry

        lax.fori_loop(0, nz, one, 0)

    from_below(collect)

    def merge(p, carry):
        stats = [own_stat[p]]
        used = [None]
        slots = [None]
        for c in range(columns):
            slot = slot_of[p * columns + c]
            used.append(slot >= 0)
            slots.append(jnp.maximum(slot, 0))
            stats.append(stat_buf[slots[-1]])
        tops = [stats[0][:1]] + [
            jnp.where(used[i], stats[i][:1], -1e30) for i in range(1, columns + 1)]
        largest = functools.reduce(jnp.maximum, tops)
        factor = jnp.exp2(tops[0] - largest)
        numer = factor * own_part[p].astype(jnp.float32)
        denom = factor * stats[0][1:]
        for i in range(1, columns + 1):
            factor = jnp.exp2(tops[i] - largest)
            numer += jnp.where(used[i], factor * part_buf[slots[i]].astype(jnp.float32), 0.0)
            denom += jnp.where(used[i], factor * stats[i][1:], 0.0)
        gathered[head_at, p] = (numer / denom).T.astype(jnp.bfloat16)
        return carry

    sends = []

    def start(copy):
        copy.start()
        sends.append(copy)

    lax.fori_loop(0, heads, merge, 0)
    start(hop(head_at, 0, right, 0))
    start(pass_over(head_at, 0, 0))
    lax.fori_loop(heads, 2 * heads, merge, 0)
    start(hop(head_at, 1, left, 1))
    start(hop(head_at, 1, right, 2))
    start(hop(head_at, 0, left, 3))
    start(pass_over(head_at, 1, 1))
    project(head_at, 0)
    project(head_at, 1)
    for n, (g, b, onward, k, k_next) in enumerate(arrivals):
        hop(g, b, right, k).wait_recv()
        if onward is not None:
            start(hop(g, b, onward, k_next))
        start(pass_over(g, b, 2 + n))
        project(g, b)
    pl.when(leads)(project_mates)
    out_ref[...] = total[...].astype(out_ref.dtype)

    def drain_below(row):
        ask_copy(row).wait_send()
        query_copy(row).wait_send()

    def drain_above(row):
        def one(at, carry):
            part_copy(row, at).wait_send()
            stat_copy(row, at).wait_send()
            return carry

        lax.fori_loop(0, nz, one, 0)

    from_below(drain_below)
    from_above(drain_above)
    for way in (0, 1):
        for step in range(half):
            if step < half - 1 or way == 0:
                key_copy(way, step).wait_send()
            if step < half - 1 or way == 1:
                value_copy(way, step).wait_send()
    for copy in sends:
        copy.wait_send()


def attend_and_project(slot_of, requests, query_rows, key_rows, value_rows, out_weight, rings,
                       groups, heads, pairs):
    ny, nz = rings
    tok_rows, feature = query_rows.shape
    width = feature // heads
    rows = tok_rows * heads // pairs
    slots = ny * nz * CAP
    vmem = pl.BlockSpec(memory_space=pltpu.VMEM)
    smem = pl.BlockSpec(memory_space=pltpu.SMEM)
    dma = pltpu.SemaphoreType.DMA
    bf16, f32, i32 = jnp.bfloat16, jnp.float32, jnp.int32
    return pl.pallas_call(
        functools.partial(main_kernel, rings),
        out_shape=jax.ShapeDtypeStruct((tok_rows, out_weight.shape[1]), bf16),
        in_specs=[smem, vmem, vmem, vmem, vmem, pl.BlockSpec(memory_space=pl.ANY)],
        out_specs=vmem,
        scratch_shapes=[
            pltpu.VMEM((ny, pairs, rows, width), bf16),
            pltpu.VMEM((pairs, width, rows), bf16),
            pltpu.VMEM((pairs, 2, rows), f32),
            pltpu.VMEM((ny, 1, 128), i32),
            pltpu.SMEM((ny, 1, 128), i32),
            pltpu.VMEM((slots, width, rows), bf16),
            pltpu.VMEM((slots, 2, rows), f32),
            pltpu.VMEM((groups, pairs, rows, width), bf16),
            pltpu.VMEM((tok_rows, out_weight.shape[1]), f32),
            pltpu.VMEM(out_weight.shape, bf16),
        ]
        + [dma((ny,)) for _ in range(4)]
        + [dma((ny, nz)) for _ in range(4)]
        + [dma((2, nz // 2)) for _ in range(4)]
        + [dma((2,)), dma((6,)), dma((6,)), dma((8,)), dma((8,))]
        + [pltpu.SemaphoreType.REGULAR] * 2
        + [pltpu.VMEM((pairs, rows, width), bf16) for _ in range(nz)]
        + [pltpu.VMEM((pairs, width, rows), bf16) for _ in range(nz)],
        compiler_params=pltpu.CompilerParams(
            collective_id=0, has_side_effects=True, vmem_limit_bytes=60 * 1024 * 1024),
    )(slot_of, requests, query_rows, key_rows, value_rows, out_weight)


def solution(mesh):
    rings, groups = RINGS[mesh.shape["seq"]], mesh.shape["head"]

    def body(query_rows, key_rows, value_rows, block_picks, out_weight):
        blocks, heads, _ = block_picks.shape
        slot_of, requests = plan(block_picks, rings)
        return attend_and_project(slot_of, requests[:, None], query_rows, key_rows, value_rows,
                                  out_weight, rings, groups, heads, blocks * heads)

    return jax.shard_map(
        body,
        mesh=mesh,
        in_specs=(
            P("seq", "head"),
            P("seq", "head"),
            P("seq", "head"),
            P("seq", "head", None),
            P(None, "head"),
        ),
        out_specs=P("seq", "head"),
        check_vma=False,
    )
```

```python
import functools

import jax
import jax.numpy as jnp
from jax import lax
from jax.experimental import pallas as pl
from jax.experimental.pallas import tpu as pltpu
from jax.sharding import PartitionSpec as P

CAP = 2
RINGS = {32: (4, 8)}
LOG2E = 1.4426950408889634
MESH = pl.DeviceIdType.MESH


def tile_partial(query, key, value_t, causal):
    scale = query.shape[-1] ** (-0.5) * LOG2E
    scores = lax.dot_general(
        key, query, (((1,), (1,)), ((), ())), preferred_element_type=jnp.float32
    )
    if causal:
        key_at = lax.broadcasted_iota(jnp.int32, scores.shape, 0)
        query_at = lax.broadcasted_iota(jnp.int32, scores.shape, 1)
        scores = jnp.where(key_at <= query_at, scores, -1e30)
    top = jnp.max(scores, axis=0, keepdims=True)
    shifted = jnp.exp2((scores - top) * scale)
    total = jnp.sum(shifted, axis=0, keepdims=True)
    part = jnp.dot(value_t, shifted.astype(jnp.bfloat16), preferred_element_type=jnp.float32)
    return part.astype(jnp.bfloat16), jnp.concatenate([top * scale, total], axis=0)


def main_kernel(
    rings,
    picks,
    q_hbm,
    k_hbm,
    v_hbm,
    w_hbm,
    out_ref,
    queries,
    v_tiles,
    own_part,
    own_stat,
    asks,
    asks_sm,
    part_buf,
    stat_buf,
    gathered,
    total,
    w_ref,
    ask_s,
    ask_r,
    q_s,
    q_r,
    part_s,
    part_r,
    stat_s,
    stat_r,
    key_s,
    key_r,
    value_s,
    value_r,
    local_sem,
    tile_sem,
    ring_s,
    ring_r,
    mate_s,
    mate_r,
    q_go,
    ring_go,
    *chunks,
):
    ny, nz = rings
    _, pairs, rows, width = queries.shape
    blocks, heads, columns = picks.shape
    entries = pairs * columns
    slots = ny * nz * CAP
    groups = gathered.shape[0]
    half = nz // 2
    keys, values_t = chunks[:nz], chunks[nz:]
    held = [[0] + [way * (half - 1) + step for step in range(1, half)] + [nz - 1]
            for way in (0, 1)]
    me = lax.axis_index("seq")
    y, z = me // nz, me % nz
    head_at = lax.axis_index("head")
    mate = head_at + 1 - 2 * (head_at % 2)
    right = (head_at + 2) % groups
    left = (head_at + groups - 2) % groups
    across = (head_at + 4) % groups
    leads = head_at % 2 == 0
    follows = head_at % 2 == 1

    def remote(src, dst, send_sem, recv_sem, to):
        return pltpu.make_async_remote_copy(
            src_ref=src, dst_ref=dst, send_sem=send_sem, recv_sem=recv_sem, device_id=to,
            device_id_type=MESH)

    def along_y(row):
        return {"seq": row * nz + z}

    def ask_copy(row):
        return remote(asks.at[y], asks.at[y], ask_s.at[row], ask_r.at[y], along_y(row))

    def query_copy(row):
        return remote(queries.at[y], queries.at[y], q_s.at[row], q_r.at[y], along_y(row))

    def part_copy(row, at, s):
        n = at * CAP + s
        return remote(part_buf.at[row * nz * CAP + n], part_buf.at[y * nz * CAP + n],
                      part_s.at[row, n], part_r.at[y, n], along_y(row))

    def stat_copy(row, at):
        src = stat_buf.at[pl.ds((row * nz + at) * CAP, CAP)]
        dst = stat_buf.at[pl.ds((y * nz + at) * CAP, CAP)]
        return remote(src, dst, stat_s.at[row, at], stat_r.at[y, at], along_y(row))

    def ring_copy(bufs, sems, way, step):
        turn = 1 - 2 * way
        to = {"seq": y * nz + (z + nz + turn) % nz}
        return remote(bufs[held[way][step]], bufs[held[way][step + 1]], sems[0].at[way, step],
                      sems[1].at[way, step], to)

    def key_copy(way, step):
        return ring_copy(keys, (key_s, key_r), way, step)

    def value_copy(way, step):
        return ring_copy(values_t, (value_s, value_r), way, step)

    def from_below(body):
        def step(row, carry):
            @pl.when(row < y)
            def _():
                body(row)

            return carry

        lax.fori_loop(0, ny, step, 0)

    def from_above(body):
        def step(row, carry):
            @pl.when(row > y)
            def _():
                body(row)

            return carry

        lax.fori_loop(0, ny, step, 0)

    def fetch(kind, p):
        b, h = p // heads, p % heads
        src = (k_hbm, q_hbm, v_hbm)[kind]
        dst = (keys[0], queries.at[y], v_tiles)[kind]
        return pltpu.make_async_copy(
            src.at[pl.ds(b * rows, rows), pl.ds(h * width, width)], dst.at[p],
            tile_sem.at[kind, p])

    asks[...] = jnp.zeros_like(asks)
    barrier = pltpu.get_barrier_semaphore()
    for step in range(1, ny):
        pl.semaphore_signal(barrier, inc=1, device_id=along_y((y + step) % ny),
                            device_id_type=MESH)
    for step in (1, nz - 1):
        pl.semaphore_signal(barrier, inc=1, device_id={"seq": y * nz + (z + step) % nz},
                            device_id_type=MESH)
    for other in (mate, right, left):
        pl.semaphore_signal(barrier, inc=1, device_id={"head": other}, device_id_type=MESH)
    for kind in range(3):
        for p in range(pairs):
            fetch(kind, p).start()
    w_copy = pltpu.make_async_copy(w_hbm, w_ref, local_sem.at[0])
    w_copy.start()

    lane = lax.broadcasted_iota(jnp.int32, (1, 128), 1)

    def owners_of(pair):
        b, h = pair // heads, pair % heads
        named = [picks[b, h, c] for c in range(columns)]
        found = []
        for c in range(columns):
            fresh = named[c] >= 0
            for earlier in range(c):
                fresh = fresh & (named[c] != named[earlier])
            block = jnp.maximum(named[c], 0)
            found.append((jnp.where(fresh, block // blocks, -1), block % blocks * heads + h))
        return found

    def place(pair, carry):
        wanted, used, owner_at = carry
        for c, (owner, code) in enumerate(owners_of(pair)):
            of_owner = lane % slots // CAP == owner
            hit = of_owner & (lane % CAP == used)
            wanted = jnp.where(hit, jnp.where(lane < slots, code, pair), wanted)
            used = jnp.where(of_owner, used + 1, used)
            owner_at = jnp.where(lane == pair * columns + c, owner, owner_at)
        return wanted, used, owner_at

    none = jnp.zeros((1, 128), jnp.int32)
    wanted, _, owner_at = lax.fori_loop(0, pairs, place, (none, none, none - 1))
    asks[y] = wanted

    def rank(pair, earlier):
        for c, (owner, _) in enumerate(owners_of(pair)):
            earlier += jnp.where((owner_at == owner) & (lane > pair * columns + c), 1, 0)
        return earlier

    ranks = lax.fori_loop(0, pairs, rank, none)
    asks[ny] = jnp.where(owner_at >= 0, owner_at * CAP + ranks, -1)
    for p in range(pairs):
        fetch(0, p).wait()
    pl.semaphore_wait(barrier, ny - 1 + 2 + 3)

    def start_queries():
        from_below(lambda row: query_copy(row).start())

    def start_ring():
        for way in (0, 1):
            key_copy(way, 0).start()
        for way in (0, 1):
            value_copy(way, 0).start()

    from_below(lambda row: ask_copy(row).start())

    @pl.when(leads)
    def _():
        key_copy(0, 0).start()
        key_copy(1, 0).start()

    for p in range(pairs):
        fetch(1, p).wait()

    @pl.when(leads)
    def _():
        start_queries()

    for p in range(pairs):
        fetch(2, p).wait()
        values_t[0][p] = v_tiles[p].T

    @pl.when(leads)
    def _():
        value_copy(0, 0).start()
        value_copy(1, 0).start()

    def own(p, carry):
        own_part[p], own_stat[p] = tile_partial(
            queries[y, p], keys[0][p], values_t[0][p], True)
        return carry

    lax.fori_loop(0, pairs, own, 0)
    total[...] = jnp.zeros_like(total)
    w_copy.wait()

    @pl.when(follows)
    def _():
        pl.semaphore_wait(q_go, 1)
        start_queries()
        pl.semaphore_wait(ring_go, 1)
        start_ring()

    from_above(lambda row: remote(
        asks.at[row], asks.at[row], ask_s.at[row], ask_r.at[row], along_y(row)).wait_recv())
    ask_copy_in = pltpu.make_async_copy(asks, asks_sm, local_sem.at[1])
    ask_copy_in.start()
    ask_copy_in.wait()

    def serve_row(row, at, n):
        for s in range(CAP):
            lane_of = (y * nz + at) * CAP + s
            code = asks_sm[row, 0, lane_of]
            pair = asks_sm[row, 0, slots + lane_of]
            i = (row * nz + at) * CAP + s
            part_buf[i], stat_buf[i] = tile_partial(
                queries[row, pair], keys[n][code], values_t[n][code], False)

            @pl.when(row > y)
            def _():
                part_copy(row, at, s).start()

    def serve(at, n):
        def one(i, carry):
            row = ny - 1 - i

            @pl.when((row > y) | ((row == y) & (at < z)))
            def _():
                serve_row(row, at, n)

            @pl.when(row > y)
            def _():
                stat_copy(row, at).start()

            return carry

        lax.fori_loop(0, ny, one, 0)

    for step in range(1, half):
        for copy_of, last_way in ((key_copy, 0), (value_copy, 1)):
            for way in (0, 1):
                copy_of(way, step - 1).wait_recv()
                if step < half - 1 or way == last_way:
                    copy_of(way, step).start()
        if step == 1:
            @pl.when(leads)
            def _():
                pl.semaphore_signal(q_go, inc=1, device_id={"head": mate}, device_id_type=MESH)

            from_above(lambda row: remote(
                queries.at[row], queries.at[row], q_s.at[row], q_r.at[row],
                along_y(row)).wait_recv())
            serve(z, 0)
        if step == half - 2:
            @pl.when(leads)
            def _():
                pl.semaphore_signal(ring_go, inc=1, device_id={"head": mate}, device_id_type=MESH)

        serve((z + nz - step) % nz, held[0][step])
        serve((z + step) % nz, held[1][step])
    parts = 2 * blocks
    tiles_in = pairs // parts

    def unit(g, u):
        return gathered.at[g, pl.ds(u * tiles_in, tiles_in)]

    def hop(g, u, way, k):
        return remote(unit(g, u), unit(g, u), ring_s.at[way, k], ring_r.at[way, k],
                      {"head": (right, left)[way]})

    def pass_over(g, u, k):
        return remote(unit(g, u), unit(g, u), mate_s.at[k], mate_r.at[k], {"head": mate})

    def project(g, u):
        tiles = jnp.concatenate(
            [gathered[g, u * tiles_in + t] for t in range(tiles_in)], axis=1)
        depth = tiles_in * width
        at = pl.multiple_of(g * heads * width + u % 2 * depth, depth)
        rows_of = pl.ds(u // 2 * rows, rows)
        total[rows_of, :] += jnp.dot(
            tiles, w_ref[pl.ds(at, depth), :], preferred_element_type=jnp.float32)

    orders = ((0, 1, 2, 3), (2, 3, 0, 1))
    arrivals = [((left, right)[way], orders[way][k], way, k) for k in range(parts)
                for way in (0, 1)]
    arrivals += [(across, orders[way][k], way, parts + k) for k in (0, 1) for way in (0, 1)]
    flip = 1 - 2 * (head_at % 2)

    def project_mates():
        for u in (0, 2, 1, 3):
            pass_over(mate, u, u).wait_recv()
            project(mate, u)
        for n, (g, u, _, _) in enumerate(arrivals):
            pass_over(g + flip, u, parts + n).wait_recv()
            project(g + flip, u)

    pl.when(follows)(project_mates)
    key_copy(0, half - 1).wait_recv()
    value_copy(1, half - 1).wait_recv()
    serve((z + half) % nz, nz - 1)

    def collect(row):
        def one(n, carry):
            here = part_buf.at[row * nz * CAP + n]
            remote(here, here, part_s.at[row, n], part_r.at[row, n], along_y(row)).wait_recv()
            return carry

        def other(at, carry):
            here = stat_buf.at[pl.ds((row * nz + at) * CAP, CAP)]
            remote(here, here, stat_s.at[row, at], stat_r.at[row, at], along_y(row)).wait_recv()
            return carry

        lax.fori_loop(0, nz * CAP, one, 0)
        lax.fori_loop(0, nz, other, 0)

    from_below(collect)

    def merge(p, carry):
        stats = [own_stat[p]]
        used = [None]
        slots = [None]
        for c in range(columns):
            slot = asks_sm[ny, 0, p * columns + c]
            used.append(slot >= 0)
            slots.append(jnp.maximum(slot, 0))
            stats.append(stat_buf[slots[-1]])
        tops = [stats[0][:1]] + [
            jnp.where(used[i], stats[i][:1], -1e30) for i in range(1, columns + 1)]
        largest = functools.reduce(jnp.maximum, tops)
        factor = jnp.exp2(tops[0] - largest)
        numer = factor * own_part[p].astype(jnp.float32)
        denom = factor * stats[0][1:]
        for i in range(1, columns + 1):
            factor = jnp.exp2(tops[i] - largest)
            numer += jnp.where(used[i], factor * part_buf[slots[i]].astype(jnp.float32), 0.0)
            denom += jnp.where(used[i], factor * stats[i][1:], 0.0)
        gathered[head_at, p] = (numer * (1.0 / denom)).astype(jnp.bfloat16).T
        return carry

    sends = []

    def start(copy):
        copy.start()
        sends.append(copy)

    for u, way in ((0, 0), (2, 1), (1, 0), (3, 1)):
        lax.fori_loop(u * tiles_in, (u + 1) * tiles_in, merge, 0)
        start(hop(head_at, u, way, u % 2))
        start(pass_over(head_at, u, u))
    for u, way in ((2, 0), (0, 1), (3, 0), (1, 1)):
        start(hop(head_at, u, way, 2 + u % 2))
    for u in range(parts):
        project(head_at, u)
    for n, (g, u, way, k) in enumerate(arrivals):
        hop(g, u, way, k).wait_recv()
        if k < 2:
            start(hop(g, u, way, parts + k))
        start(pass_over(g, u, parts + n))
        project(g, u)
    pl.when(leads)(project_mates)
    out_ref[...] = total[...].astype(out_ref.dtype)

    def drain_below(row):
        ask_copy(row).wait_send()
        query_copy(row).wait_send()

    def drain_above(row):
        def one(at, carry):
            for s in range(CAP):
                part_copy(row, at, s).wait_send()
            stat_copy(row, at).wait_send()
            return carry

        lax.fori_loop(0, nz, one, 0)

    from_below(drain_below)
    from_above(drain_above)
    for way in (0, 1):
        for step in range(half):
            if step < half - 1 or way == 0:
                key_copy(way, step).wait_send()
            if step < half - 1 or way == 1:
                value_copy(way, step).wait_send()
    for copy in sends:
        copy.wait_send()


def attend_and_project(picks, query_rows, key_rows, value_rows, out_weight, rings, groups):
    ny, nz = rings
    blocks, heads, _ = picks.shape
    tok_rows, feature = query_rows.shape
    width, rows, pairs = feature // heads, tok_rows // blocks, blocks * heads
    slots = ny * nz * CAP
    hbm = pl.BlockSpec(memory_space=pl.ANY)
    dma = pltpu.SemaphoreType.DMA
    bf16, f32, i32 = jnp.bfloat16, jnp.float32, jnp.int32
    return pl.pallas_call(
        functools.partial(main_kernel, rings),
        out_shape=jax.ShapeDtypeStruct((tok_rows, out_weight.shape[1]), bf16),
        in_specs=[pl.BlockSpec(memory_space=pltpu.SMEM), hbm, hbm, hbm, hbm],
        out_specs=pl.BlockSpec(memory_space=pltpu.VMEM),
        scratch_shapes=[
            pltpu.VMEM((ny, pairs, rows, width), bf16),
            pltpu.VMEM((pairs, rows, width), bf16),
            pltpu.VMEM((pairs, width, rows), bf16),
            pltpu.VMEM((pairs, 2, rows), f32),
            pltpu.VMEM((ny + 1, 1, 128), i32),
            pltpu.SMEM((ny + 1, 1, 128), i32),
            pltpu.VMEM((slots, width, rows), bf16),
            pltpu.VMEM((slots, 2, rows), f32),
            pltpu.VMEM((groups, pairs, rows, width), bf16),
            pltpu.VMEM((tok_rows, out_weight.shape[1]), f32),
            pltpu.VMEM(out_weight.shape, bf16),
        ]
        + [dma((ny,)) for _ in range(4)]
        + [dma((ny, nz * CAP)) for _ in range(2)]
        + [dma((ny, nz)) for _ in range(2)]
        + [dma((2, nz // 2)) for _ in range(4)]
        + [dma((2,)), dma((3, pairs)), dma((2, 6)), dma((2, 6)), dma((16,)), dma((16,))]
        + [pltpu.SemaphoreType.REGULAR] * 2
        + [pltpu.VMEM((pairs, rows, width), bf16) for _ in range(nz)]
        + [pltpu.VMEM((pairs, width, rows), bf16) for _ in range(nz)],
        compiler_params=pltpu.CompilerParams(
            collective_id=0, has_side_effects=True, vmem_limit_bytes=60 * 1024 * 1024),
    )(picks, query_rows, key_rows, value_rows, out_weight)


def solution(mesh):
    rings, groups = RINGS[mesh.shape["seq"]], mesh.shape["head"]

    def body(query_rows, key_rows, value_rows, block_picks, out_weight):
        return attend_and_project(
            block_picks, query_rows, key_rows, value_rows, out_weight, rings, groups)

    return jax.shard_map(
        body,
        mesh=mesh,
        in_specs=(
            P("seq", "head"),
            P("seq", "head"),
            P("seq", "head"),
            P("seq", "head", None),
            P(None, "head"),
        ),
        out_specs=P("seq", "head"),
        check_vma=False,
    )
```

```python
import functools

import jax
import jax.numpy as jnp
from jax import lax
from jax.experimental import pallas as pl
from jax.experimental.pallas import tpu as pltpu
from jax.sharding import PartitionSpec as P

CAP = 2
LENT = 2
RINGS = {32: (4, 8)}
LOG2E = 1.4426950408889634
MESH = pl.DeviceIdType.MESH


def tile_partial(query, key, value_t, causal):
    scale = query.shape[-1] ** (-0.5) * LOG2E
    scores = lax.dot_general(
        key, query, (((1,), (1,)), ((), ())), preferred_element_type=jnp.float32
    )
    if causal:
        key_at = lax.broadcasted_iota(jnp.int32, scores.shape, 0)
        query_at = lax.broadcasted_iota(jnp.int32, scores.shape, 1)
        scores = jnp.where(key_at <= query_at, scores, -1e30)
    top = jnp.max(scores, axis=0, keepdims=True)
    shifted = jnp.exp2((scores - top) * scale)
    total = jnp.sum(shifted, axis=0, keepdims=True)
    part = jnp.dot(value_t, shifted.astype(jnp.bfloat16), preferred_element_type=jnp.float32)
    return part.astype(jnp.bfloat16), jnp.concatenate([top * scale, total], axis=0)


def main_kernel(
    rings,
    picks,
    q_hbm,
    k_hbm,
    v_hbm,
    w_hbm,
    out_ref,
    queries,
    v_tiles,
    own_part,
    own_stat,
    asks,
    asks_sm,
    part_buf,
    stat_buf,
    gathered,
    total,
    w_ref,
    ask_s,
    ask_r,
    q_s,
    q_r,
    part_s,
    part_r,
    stat_s,
    stat_r,
    key_s,
    key_r,
    value_s,
    value_r,
    local_sem,
    tile_sem,
    ring_s,
    ring_r,
    mate_s,
    mate_r,
    q_go,
    ring_go,
    guests,
    slot_queries,
    row_ask_s,
    row_ask_r,
    slot_q_s,
    slot_q_r,
    lend_s,
    lend_r,
    guest_s,
    guest_r,
    back_s,
    back_r,
    *chunks,
):
    ny, nz = rings
    _, pairs, rows, width = queries.shape
    blocks, heads, columns = picks.shape
    entries = pairs * columns
    slots = ny * nz * CAP
    groups = gathered.shape[0]
    half = nz // 2
    keys, values_t = chunks[:nz], chunks[nz:]
    held = [[0] + [way * (half - 1) + step for step in range(1, half)] + [nz - 1]
            for way in (0, 1)]
    me = lax.axis_index("seq")
    y, z = me // nz, me % nz
    head_at = lax.axis_index("head")
    mate = head_at + 1 - 2 * (head_at % 2)
    right = (head_at + 2) % groups
    left = (head_at + groups - 2) % groups
    across = (head_at + 4) % groups
    leads = head_at % 2 == 0
    follows = head_at % 2 == 1
    last = ny - 1
    kept = pairs - LENT
    in_ring = y < last
    helps = y == last

    def remote(src, dst, send_sem, recv_sem, to):
        return pltpu.make_async_remote_copy(
            src_ref=src, dst_ref=dst, send_sem=send_sem, recv_sem=recv_sem, device_id=to,
            device_id_type=MESH)

    def along_y(row):
        return {"seq": row * nz + z}

    def ask_copy(row):
        return remote(asks.at[y], asks.at[y], ask_s.at[row], ask_r.at[y], along_y(row))

    def query_copy(row):
        return remote(queries.at[y], queries.at[y], q_s.at[row], q_r.at[y], along_y(row))

    def part_copy(row, at, s):
        n = at * CAP + s
        return remote(part_buf.at[row * nz * CAP + n], part_buf.at[y * nz * CAP + n],
                      part_s.at[row, n], part_r.at[y, n], along_y(row))

    def stat_copy(row, at):
        src = stat_buf.at[pl.ds((row * nz + at) * CAP, CAP)]
        dst = stat_buf.at[pl.ds((y * nz + at) * CAP, CAP)]
        return remote(src, dst, stat_s.at[row, at], stat_r.at[y, at], along_y(row))

    def along_z(at):
        return {"seq": y * nz + at}

    def ring_to(way):
        return along_z((z + nz + 1 - 2 * way) % nz)

    def key_copy(way, step):
        here, there = keys[held[way][step]], keys[held[way][step + 1]]
        span = pl.ds(0, pairs)
        if step == half - 1:
            span = (pl.ds(0, pairs - 1), pl.ds(pairs - 1, 1))[way]
        return remote(here.at[span], there.at[span], key_s.at[way, step], key_r.at[way, step],
                      ring_to(way))

    def value_copy(way, step):
        here, there = values_t[held[way][step]], values_t[held[way][step + 1]]
        span = pl.ds(0, kept)
        return remote(here.at[span], there.at[span], value_s.at[way, step],
                      value_r.at[way, step], ring_to(way))

    def guest(n, row, first=0, size=LENT):
        span = pl.ds(row * LENT + first, size)
        return guests.at[span] if n == 0 else values_t[n].at[span]

    def lend_copy(row):
        return remote(values_t[0].at[pl.ds(kept, LENT)], guest(0, row), lend_s.at[0],
                      lend_r.at[row], along_y(last))

    def guest_copy(row, way, step):
        cut = (0, LENT) if step < half - 1 else (way * (LENT // 2), LENT // 2)
        return remote(guest(held[way][step], row, *cut), guest(held[way][step + 1], row, *cut),
                      guest_s.at[row, way, step], guest_r.at[row, way, step], ring_to(way))

    def back_copy(row, n):
        return remote(guest(n, row), values_t[n].at[pl.ds(kept, LENT)], back_s.at[row, n],
                      back_r.at[n], along_y(row))

    def row_ask_copy(at):
        return remote(asks.at[y], asks.at[ny + 1 + z], row_ask_s.at[at], row_ask_r.at[z],
                      along_z(at))

    def slot_query_copy(at):
        return remote(slot_queries.at[pl.ds(at * CAP, CAP)],
                      slot_queries.at[pl.ds(z * CAP, CAP)], slot_q_s.at[at], slot_q_r.at[z],
                      along_z(at))

    def row_part_copy(at, s):
        return remote(part_buf.at[(y * nz + at) * CAP + s], part_buf.at[(y * nz + z) * CAP + s],
                      part_s.at[y, at * CAP + s], part_r.at[y, z * CAP + s], along_z(at))

    def row_stat_copy(at):
        return remote(stat_buf.at[pl.ds((y * nz + at) * CAP, CAP)],
                      stat_buf.at[pl.ds((y * nz + z) * CAP, CAP)], stat_s.at[y, at],
                      stat_r.at[y, z], along_z(at))

    def over(low, high, body):
        def step(at, carry):
            body(at)
            return carry

        lax.fori_loop(low, high, step, 0)

    def from_below(body):
        def step(row, carry):
            @pl.when(row < y)
            def _():
                body(row)

            return carry

        lax.fori_loop(0, ny, step, 0)

    def from_above(body):
        def step(row, carry):
            @pl.when(row > y)
            def _():
                body(row)

            return carry

        lax.fori_loop(0, ny, step, 0)

    def fetch(kind, p):
        b, h = p // heads, p % heads
        src = (k_hbm, q_hbm, v_hbm)[kind]
        dst = (keys[0], queries.at[y], v_tiles)[kind]
        return pltpu.make_async_copy(
            src.at[pl.ds(b * rows, rows), pl.ds(h * width, width)], dst.at[p],
            tile_sem.at[kind, p])

    asks[...] = jnp.zeros_like(asks)
    barrier = pltpu.get_barrier_semaphore()
    for step in range(1, ny):
        pl.semaphore_signal(barrier, inc=1, device_id=along_y((y + step) % ny),
                            device_id_type=MESH)
    for step in range(1, nz):
        pl.semaphore_signal(barrier, inc=1, device_id=along_z((z + step) % nz),
                            device_id_type=MESH)
    for other in (mate, right, left):
        pl.semaphore_signal(barrier, inc=1, device_id={"head": other}, device_id_type=MESH)
    for kind in range(3):
        for p in range(pairs):
            fetch(kind, p).start()
    w_copy = pltpu.make_async_copy(w_hbm, w_ref, local_sem.at[0])
    w_copy.start()

    lane = lax.broadcasted_iota(jnp.int32, (1, 128), 1)

    def owners_of(pair):
        b, h = pair // heads, pair % heads
        named = [picks[b, h, c] for c in range(columns)]
        found = []
        for c in range(columns):
            fresh = named[c] >= 0
            for earlier in range(c):
                fresh = fresh & (named[c] != named[earlier])
            block = jnp.maximum(named[c], 0)
            found.append((jnp.where(fresh, block // blocks, -1), block % blocks * heads + h))
        return found

    def place(pair, carry):
        wanted, used, owner_at = carry
        for c, (owner, code) in enumerate(owners_of(pair)):
            of_owner = lane % slots // CAP == owner
            hit = of_owner & (lane % CAP == used)
            wanted = jnp.where(hit, jnp.where(lane < slots, code, pair), wanted)
            used = jnp.where(of_owner, used + 1, used)
            owner_at = jnp.where(lane == pair * columns + c, owner, owner_at)
        return wanted, used, owner_at

    none = jnp.zeros((1, 128), jnp.int32)
    wanted, _, owner_at = lax.fori_loop(0, pairs, place, (none, none, none - 1))
    asks[y] = wanted

    def rank(pair, earlier):
        for c, (owner, _) in enumerate(owners_of(pair)):
            earlier += jnp.where((owner_at == owner) & (lane > pair * columns + c), 1, 0)
        return earlier

    ranks = lax.fori_loop(0, pairs, rank, none)
    asks[ny] = jnp.where(owner_at >= 0, owner_at * CAP + ranks, -1)
    for p in range(pairs):
        fetch(0, p).wait()
    pl.semaphore_wait(barrier, ny - 1 + nz - 1 + 3)

    def start_queries():
        from_below(lambda row: query_copy(row).start())

    def start_ring():
        for way in (0, 1):
            key_copy(way, 0).start()
        for way in (0, 1):
            value_copy(way, 0).start()

    from_below(lambda row: ask_copy(row).start())

    @pl.when(leads & in_ring)
    def _():
        key_copy(0, 0).start()
        key_copy(1, 0).start()

    @pl.when(helps)
    def _():
        over(0, z, lambda at: row_ask_copy(at).start())

    for p in range(pairs):
        fetch(1, p).wait()

    @pl.when(leads)
    def _():
        start_queries()

    for p in range(pairs):
        fetch(2, p).wait()
        values_t[0][p] = v_tiles[p].T

    @pl.when(in_ring)
    def _():
        lend_copy(y).start()

    @pl.when(leads & in_ring)
    def _():
        value_copy(0, 0).start()
        value_copy(1, 0).start()

    def begin_guests():
        def begin(row):
            remote(guest(0, row), guest(0, row), lend_s.at[0], lend_r.at[row],
                   along_y(row)).wait_recv()
            for way in (0, 1):
                guest_copy(row, way, 0).start()

        over(0, last, begin)

    pl.when(leads & helps)(begin_guests)

    def own(p, carry):
        own_part[p], own_stat[p] = tile_partial(
            queries[y, p], keys[0][p], values_t[0][p], True)
        return carry

    lax.fori_loop(0, pairs, own, 0)

    def greenlight(sem):
        pl.semaphore_signal(sem, inc=1, device_id={"head": mate}, device_id_type=MESH)

    @pl.when(leads & helps)
    def _():
        greenlight(q_go)

    total[...] = jnp.zeros_like(total)
    w_copy.wait()

    @pl.when(follows)
    def _():
        pl.semaphore_wait(q_go, 1)
        start_queries()
        pl.semaphore_wait(ring_go, 1)
        pl.when(in_ring)(start_ring)
        pl.when(helps)(begin_guests)

    from_above(lambda row: remote(
        asks.at[row], asks.at[row], ask_s.at[row], ask_r.at[row], along_y(row)).wait_recv())

    @pl.when(helps)
    def _():
        over(z + 1, nz, lambda at: remote(
            asks.at[ny + 1 + at], asks.at[ny + 1 + at], row_ask_s.at[at], row_ask_r.at[at],
            along_z(at)).wait_recv())

    ask_copy_in = pltpu.make_async_copy(asks, asks_sm, local_sem.at[1])
    ask_copy_in.start()
    ask_copy_in.wait()

    def serve_row(row, at, n):
        for s in range(CAP):
            lane_of = (y * nz + at) * CAP + s
            code = asks_sm[row, 0, lane_of]
            pair = asks_sm[row, 0, slots + lane_of]
            i = (row * nz + at) * CAP + s
            part_buf[i], stat_buf[i] = tile_partial(
                queries[row, pair], keys[n][code], values_t[n][code], False)

            @pl.when(row > y)
            def _():
                part_copy(row, at, s).start()

    def serve(at, n):
        def one(i, carry):
            row = ny - 1 - i

            @pl.when((row > y) | ((row == y) & (at < z)))
            def _():
                serve_row(row, at, n)

            @pl.when(row > y)
            def _():
                stat_copy(row, at).start()

            return carry

        lax.fori_loop(0, ny, one, 0)

    def take_back(n):
        here = values_t[n].at[pl.ds(kept, LENT)]
        remote(here, here, back_s.at[0, n], back_r.at[n], along_y(last)).wait_recv()

    def serve_both(step):
        for way, at in ((0, (z + nz - step) % nz), (1, (z + step) % nz)):
            take_back(held[way][step])
            serve(at, held[way][step])

    @pl.when(in_ring)
    def _():
        for step in range(1, half):
            for copy_of, final in ((key_copy, (0, 1)), (value_copy, (1,))):
                for way in (0, 1):
                    copy_of(way, step - 1).wait_recv()
                    if step < half - 1 or way in final:
                        copy_of(way, step).start()
            if step == 1:
                @pl.when(leads)
                def _():
                    greenlight(q_go)

                from_above(lambda row: remote(
                    queries.at[row], queries.at[row], q_s.at[row], q_r.at[row],
                    along_y(row)).wait_recv())
                serve(z, 0)
            if step == half - 2:
                @pl.when(leads)
                def _():
                    greenlight(ring_go)

            if step > 1:
                serve_both(step - 1)
        serve_both(half - 1)

    @pl.when(helps)
    def _():
        for step in range(1, half):
            def onward(row):
                for way in (0, 1):
                    guest_copy(row, way, step - 1).wait_recv()
                    guest_copy(row, way, step).start()
                    back_copy(row, held[way][step]).start()

            over(0, last, onward)

        def finish(row):
            for way in (0, 1):
                guest_copy(row, way, half - 1).wait_recv()
            back_copy(row, nz - 1).start()

        over(0, last, finish)

        @pl.when(leads)
        def _():
            greenlight(ring_go)

        def ask_slot(at):
            for s in range(CAP):
                lane_of = (y * nz + at) * CAP + s
                slot_queries[at * CAP + s] = queries[y, asks_sm[y, 0, slots + lane_of]]

        over(0, z, ask_slot)
        over(0, z, lambda at: slot_query_copy(at).start())

        def serve_slots(at):
            here = slot_queries.at[pl.ds(at * CAP, CAP)]
            remote(here, here, slot_q_s.at[at], slot_q_r.at[at], along_z(at)).wait_recv()
            for s in range(CAP):
                code = asks_sm[ny + 1 + at, 0, (y * nz + z) * CAP + s]
                i = (y * nz + at) * CAP + s
                part_buf[i], stat_buf[i] = tile_partial(
                    slot_queries[at * CAP + s], keys[0][code], values_t[0][code], False)
                row_part_copy(at, s).start()
            row_stat_copy(at).start()

        over(z + 1, nz, serve_slots)

    parts = 2 * blocks
    tiles_in = pairs // parts

    def unit(g, u):
        return gathered.at[g, pl.ds(u * tiles_in, tiles_in)]

    def hop(g, u, way, k):
        return remote(unit(g, u), unit(g, u), ring_s.at[way, k], ring_r.at[way, k],
                      {"head": (right, left)[way]})

    def pass_over(g, u, k):
        return remote(unit(g, u), unit(g, u), mate_s.at[k], mate_r.at[k], {"head": mate})

    def project(g, u):
        tiles = jnp.concatenate(
            [gathered[g, u * tiles_in + t] for t in range(tiles_in)], axis=1)
        depth = tiles_in * width
        at = pl.multiple_of(g * heads * width + u % 2 * depth, depth)
        rows_of = pl.ds(u // 2 * rows, rows)
        total[rows_of, :] += jnp.dot(
            tiles, w_ref[pl.ds(at, depth), :], preferred_element_type=jnp.float32)

    orders = ((0, 1, 2, 3), (2, 3, 0, 1))
    arrivals = [((left, right)[way], orders[way][k], way, k) for k in range(parts)
                for way in (0, 1)]
    arrivals += [(across, orders[way][k], way, parts + k) for k in (0, 1) for way in (0, 1)]
    flip = 1 - 2 * (head_at % 2)

    def project_mates():
        for u in (0, 2, 1, 3):
            pass_over(mate, u, u).wait_recv()
            project(mate, u)
        for n, (g, u, _, _) in enumerate(arrivals):
            pass_over(g + flip, u, parts + n).wait_recv()
            project(g + flip, u)

    @pl.when(in_ring)
    def _():
        key_copy(0, half - 1).wait_recv()
        key_copy(1, half - 1).wait_recv()
        take_back(nz - 1)
        value_copy(1, half - 1).wait_recv()
        serve((z + half) % nz, nz - 1)

    def collect(row):
        def one(n, carry):
            here = part_buf.at[row * nz * CAP + n]
            remote(here, here, part_s.at[row, n], part_r.at[row, n], along_y(row)).wait_recv()
            return carry

        def other(at, carry):
            here = stat_buf.at[pl.ds((row * nz + at) * CAP, CAP)]
            remote(here, here, stat_s.at[row, at], stat_r.at[row, at], along_y(row)).wait_recv()
            return carry

        lax.fori_loop(0, nz * CAP, one, 0)
        lax.fori_loop(0, nz, other, 0)

    pl.when(follows)(project_mates)
    from_below(collect)

    @pl.when(helps)
    def _():
        def collect_slots(at):
            for s in range(CAP):
                here = part_buf.at[(y * nz + at) * CAP + s]
                n = at * CAP + s
                remote(here, here, part_s.at[y, n], part_r.at[y, n], along_z(at)).wait_recv()
            here = stat_buf.at[pl.ds((y * nz + at) * CAP, CAP)]
            remote(here, here, stat_s.at[y, at], stat_r.at[y, at], along_z(at)).wait_recv()

        over(0, z, collect_slots)

    def merge(p, carry):
        stats = [own_stat[p]]
        used = [None]
        slots = [None]
        for c in range(columns):
            slot = asks_sm[ny, 0, p * columns + c]
            used.append(slot >= 0)
            slots.append(jnp.maximum(slot, 0))
            stats.append(stat_buf[slots[-1]])
        tops = [stats[0][:1]] + [
            jnp.where(used[i], stats[i][:1], -1e30) for i in range(1, columns + 1)]
        largest = functools.reduce(jnp.maximum, tops)
        factor = jnp.exp2(tops[0] - largest)
        numer = factor * own_part[p].astype(jnp.float32)
        denom = factor * stats[0][1:]
        for i in range(1, columns + 1):
            factor = jnp.exp2(tops[i] - largest)
            numer += jnp.where(used[i], factor * part_buf[slots[i]].astype(jnp.float32), 0.0)
            denom += jnp.where(used[i], factor * stats[i][1:], 0.0)
        gathered[head_at, p] = (numer * (1.0 / denom)).astype(jnp.bfloat16).T
        return carry

    sends = []

    def start(copy):
        copy.start()
        sends.append(copy)

    for u, way in ((0, 0), (2, 1), (1, 0), (3, 1)):
        lax.fori_loop(u * tiles_in, (u + 1) * tiles_in, merge, 0)
        start(hop(head_at, u, way, u % 2))
        start(pass_over(head_at, u, u))
    for u, way in ((2, 0), (0, 1), (3, 0), (1, 1)):
        start(hop(head_at, u, way, 2 + u % 2))
    for u in range(parts):
        project(head_at, u)
    for n, (g, u, way, k) in enumerate(arrivals):
        hop(g, u, way, k).wait_recv()
        if k < 2:
            start(hop(g, u, way, parts + k))
        start(pass_over(g, u, parts + n))
        project(g, u)
    pl.when(leads)(project_mates)
    out_ref[...] = total[...].astype(out_ref.dtype)

    def drain_below(row):
        ask_copy(row).wait_send()
        query_copy(row).wait_send()

    def drain_above(row):
        def one(at, carry):
            for s in range(CAP):
                part_copy(row, at, s).wait_send()
            stat_copy(row, at).wait_send()
            return carry

        lax.fori_loop(0, nz, one, 0)

    from_below(drain_below)
    from_above(drain_above)

    @pl.when(in_ring)
    def _():
        lend_copy(y).wait_send()
        for way in (0, 1):
            for step in range(half):
                key_copy(way, step).wait_send()
                if step < half - 1 or way == 1:
                    value_copy(way, step).wait_send()

    @pl.when(helps)
    def _():
        def drain_asks(at):
            row_ask_copy(at).wait_send()
            slot_query_copy(at).wait_send()

        def drain_parts(at):
            for s in range(CAP):
                row_part_copy(at, s).wait_send()
            row_stat_copy(at).wait_send()

        def drain_guests(row):
            for way in (0, 1):
                for step in range(half):
                    guest_copy(row, way, step).wait_send()
            for n in range(1, nz):
                back_copy(row, n).wait_send()

        over(0, z, drain_asks)
        over(z + 1, nz, drain_parts)
        over(0, last, drain_guests)

    for copy in sends:
        copy.wait_send()


def attend_and_project(picks, query_rows, key_rows, value_rows, out_weight, rings, groups):
    ny, nz = rings
    blocks, heads, _ = picks.shape
    tok_rows, feature = query_rows.shape
    width, rows, pairs = feature // heads, tok_rows // blocks, blocks * heads
    slots = ny * nz * CAP
    hbm = pl.BlockSpec(memory_space=pl.ANY)
    dma = pltpu.SemaphoreType.DMA
    bf16, f32, i32 = jnp.bfloat16, jnp.float32, jnp.int32
    return pl.pallas_call(
        functools.partial(main_kernel, rings),
        out_shape=jax.ShapeDtypeStruct((tok_rows, out_weight.shape[1]), bf16),
        in_specs=[pl.BlockSpec(memory_space=pltpu.SMEM), hbm, hbm, hbm, hbm],
        out_specs=pl.BlockSpec(memory_space=pltpu.VMEM),
        scratch_shapes=[
            pltpu.VMEM((ny, pairs, rows, width), bf16),
            pltpu.VMEM((pairs, rows, width), bf16),
            pltpu.VMEM((pairs, width, rows), bf16),
            pltpu.VMEM((pairs, 2, rows), f32),
            pltpu.VMEM((ny + 1 + nz, 1, 128), i32),
            pltpu.SMEM((ny + 1 + nz, 1, 128), i32),
            pltpu.VMEM((slots, width, rows), bf16),
            pltpu.VMEM((slots, 2, rows), f32),
            pltpu.VMEM((groups, pairs, rows, width), bf16),
            pltpu.VMEM((tok_rows, out_weight.shape[1]), f32),
            pltpu.VMEM(out_weight.shape, bf16),
        ]
        + [dma((ny,)) for _ in range(4)]
        + [dma((ny, nz * CAP)) for _ in range(2)]
        + [dma((ny, nz)) for _ in range(2)]
        + [dma((2, nz // 2)) for _ in range(4)]
        + [dma((2,)), dma((3, pairs)), dma((2, 6)), dma((2, 6)), dma((16,)), dma((16,))]
        + [pltpu.SemaphoreType.REGULAR] * 2
        + [pltpu.VMEM(((ny - 1) * LENT, width, rows), bf16),
           pltpu.VMEM((nz * CAP, rows, width), bf16)]
        + [dma((nz,)) for _ in range(4)]
        + [dma((1,)), dma((ny - 1,))]
        + [dma((ny - 1, 2, nz // 2)) for _ in range(2)]
        + [dma((ny - 1, nz)), dma((nz,))]
        + [pltpu.VMEM((pairs, rows, width), bf16) for _ in range(nz)]
        + [pltpu.VMEM((pairs, width, rows), bf16) for _ in range(nz)],
        compiler_params=pltpu.CompilerParams(
            collective_id=0, has_side_effects=True, vmem_limit_bytes=60 * 1024 * 1024),
    )(picks, query_rows, key_rows, value_rows, out_weight)


def solution(mesh):
    rings, groups = RINGS[mesh.shape["seq"]], mesh.shape["head"]

    def body(query_rows, key_rows, value_rows, block_picks, out_weight):
        return attend_and_project(
            block_picks, query_rows, key_rows, value_rows, out_weight, rings, groups)

    return jax.shard_map(
        body,
        mesh=mesh,
        in_specs=(
            P("seq", "head"),
            P("seq", "head"),
            P("seq", "head"),
            P("seq", "head", None),
            P(None, "head"),
        ),
        out_specs=P("seq", "head"),
        check_vma=False,
    )
```

```python
import functools

import jax
import jax.numpy as jnp
from jax import lax
from jax.experimental import pallas as pl
from jax.experimental.pallas import tpu as pltpu
from jax.sharding import PartitionSpec as P

CAP = 2
LENT = 2
RINGS = {32: (4, 8)}
LOG2E = 1.4426950408889634
MESH = pl.DeviceIdType.MESH


def tile_partial(query, key, value_t, causal):
    scale = query.shape[-1] ** (-0.5) * LOG2E
    scores = lax.dot_general(
        key, query, (((1,), (1,)), ((), ())), preferred_element_type=jnp.float32
    )
    if causal:
        key_at = lax.broadcasted_iota(jnp.int32, scores.shape, 0)
        query_at = lax.broadcasted_iota(jnp.int32, scores.shape, 1)
        scores = jnp.where(key_at <= query_at, scores, -1e30)
    top = jnp.max(scores, axis=0, keepdims=True)
    shifted = jnp.exp2((scores - top) * scale)
    total = jnp.sum(shifted, axis=0, keepdims=True)
    part = jnp.dot(value_t, shifted.astype(jnp.bfloat16), preferred_element_type=jnp.float32)
    return part.astype(jnp.bfloat16), jnp.concatenate([top * scale, total], axis=0)


def main_kernel(
    rings,
    picks,
    q_hbm,
    k_hbm,
    v_hbm,
    w_hbm,
    out_ref,
    queries,
    v_tiles,
    own_part,
    own_stat,
    asks,
    asks_sm,
    part_buf,
    stat_buf,
    gathered,
    total,
    w_ref,
    ask_s,
    ask_r,
    q_s,
    q_r,
    part_s,
    part_r,
    stat_s,
    stat_r,
    key_s,
    key_r,
    value_s,
    value_r,
    local_sem,
    tile_sem,
    ring_s,
    ring_r,
    mate_s,
    mate_r,
    q_go,
    ring_go,
    guests,
    slot_queries,
    row_ask_s,
    row_ask_r,
    slot_q_s,
    slot_q_r,
    lend_s,
    lend_r,
    guest_s,
    guest_r,
    back_s,
    back_r,
    *chunks,
):
    ny, nz = rings
    _, pairs, rows, width = queries.shape
    blocks, heads, columns = picks.shape
    entries = pairs * columns
    slots = ny * nz * CAP
    groups = gathered.shape[0]
    half = nz // 2
    keys, values_t = chunks[:nz], chunks[nz:]
    held = [[0] + [way * (half - 1) + step for step in range(1, half)] + [nz - 1]
            for way in (0, 1)]
    me = lax.axis_index("seq")
    y, z = me // nz, me % nz
    head_at = lax.axis_index("head")
    mate = head_at + 1 - 2 * (head_at % 2)
    right = (head_at + 2) % groups
    left = (head_at + groups - 2) % groups
    across = (head_at + 4) % groups
    leads = head_at % 2 == 0
    follows = head_at % 2 == 1
    last = ny - 1
    kept = pairs - LENT
    in_ring = y < last
    helps = y == last

    def remote(src, dst, send_sem, recv_sem, to):
        return pltpu.make_async_remote_copy(
            src_ref=src, dst_ref=dst, send_sem=send_sem, recv_sem=recv_sem, device_id=to,
            device_id_type=MESH)

    def along_y(row):
        return {"seq": row * nz + z}

    def ask_copy(row):
        return remote(asks.at[y], asks.at[y], ask_s.at[row], ask_r.at[y], along_y(row))

    def query_copy(row):
        return remote(queries.at[y], queries.at[y], q_s.at[row], q_r.at[y], along_y(row))

    def part_copy(row, at, s):
        n = at * CAP + s
        return remote(part_buf.at[row * nz * CAP + n], part_buf.at[y * nz * CAP + n],
                      part_s.at[row, n], part_r.at[y, n], along_y(row))

    def stat_copy(row, at):
        src = stat_buf.at[pl.ds((row * nz + at) * CAP, CAP)]
        dst = stat_buf.at[pl.ds((y * nz + at) * CAP, CAP)]
        return remote(src, dst, stat_s.at[row, at], stat_r.at[y, at], along_y(row))

    def along_z(at):
        return {"seq": y * nz + at}

    def ring_to(way):
        return along_z((z + nz + 1 - 2 * way) % nz)

    def key_copy(way, step):
        here, there = keys[held[way][step]], keys[held[way][step + 1]]
        span = pl.ds(0, pairs)
        if step == half - 1:
            span = (pl.ds(0, pairs - 1), pl.ds(pairs - 1, 1))[way]
        return remote(here.at[span], there.at[span], key_s.at[way, step], key_r.at[way, step],
                      ring_to(way))

    def value_copy(way, step):
        here, there = values_t[held[way][step]], values_t[held[way][step + 1]]
        span = pl.ds(0, kept)
        return remote(here.at[span], there.at[span], value_s.at[way, step],
                      value_r.at[way, step], ring_to(way))

    def guest(n, row, first=0, size=LENT):
        span = pl.ds(row * LENT + first, size)
        return guests.at[span] if n == 0 else values_t[n].at[span]

    def lend_copy(row):
        return remote(values_t[0].at[pl.ds(kept, LENT)], guest(0, row), lend_s.at[0],
                      lend_r.at[row], along_y(last))

    def guest_copy(row, way, step):
        cut = (0, LENT) if step < half - 1 else (way * (LENT // 2), LENT // 2)
        return remote(guest(held[way][step], row, *cut), guest(held[way][step + 1], row, *cut),
                      guest_s.at[row, way, step], guest_r.at[row, way, step], ring_to(way))

    def back_copy(row, n):
        return remote(guest(n, row), values_t[n].at[pl.ds(kept, LENT)], back_s.at[row, n],
                      back_r.at[n], along_y(row))

    def row_ask_copy(at):
        return remote(asks.at[y], asks.at[ny + 1 + z], row_ask_s.at[at], row_ask_r.at[z],
                      along_z(at))

    def slot_query_copy(at):
        return remote(slot_queries.at[pl.ds(at * CAP, CAP)],
                      slot_queries.at[pl.ds(z * CAP, CAP)], slot_q_s.at[at], slot_q_r.at[z],
                      along_z(at))

    def row_part_copy(at, s):
        return remote(part_buf.at[(y * nz + at) * CAP + s], part_buf.at[(y * nz + z) * CAP + s],
                      part_s.at[y, at * CAP + s], part_r.at[y, z * CAP + s], along_z(at))

    def row_stat_copy(at):
        return remote(stat_buf.at[pl.ds((y * nz + at) * CAP, CAP)],
                      stat_buf.at[pl.ds((y * nz + z) * CAP, CAP)], stat_s.at[y, at],
                      stat_r.at[y, z], along_z(at))

    def over(low, high, body):
        def step(at, carry):
            body(at)
            return carry

        lax.fori_loop(low, high, step, 0)

    def from_below(body):
        def step(row, carry):
            @pl.when(row < y)
            def _():
                body(row)

            return carry

        lax.fori_loop(0, ny, step, 0)

    def from_above(body):
        def step(row, carry):
            @pl.when(row > y)
            def _():
                body(row)

            return carry

        lax.fori_loop(0, ny, step, 0)

    def fetch(kind, p):
        b, h = p // heads, p % heads
        src = (k_hbm, q_hbm, v_hbm)[kind]
        dst = (keys[0], queries.at[y], v_tiles)[kind]
        return pltpu.make_async_copy(
            src.at[pl.ds(b * rows, rows), pl.ds(h * width, width)], dst.at[p],
            tile_sem.at[kind, p])

    asks[...] = jnp.zeros_like(asks)
    barrier = pltpu.get_barrier_semaphore()
    for step in range(1, ny):
        pl.semaphore_signal(barrier, inc=1, device_id=along_y((y + step) % ny),
                            device_id_type=MESH)
    for step in range(1, nz):
        pl.semaphore_signal(barrier, inc=1, device_id=along_z((z + step) % nz),
                            device_id_type=MESH)
    for other in (mate, right, left):
        pl.semaphore_signal(barrier, inc=1, device_id={"head": other}, device_id_type=MESH)
    for kind in range(3):
        for p in range(pairs):
            fetch(kind, p).start()
    w_copy = pltpu.make_async_copy(w_hbm, w_ref, local_sem.at[0])
    w_copy.start()

    lane = lax.broadcasted_iota(jnp.int32, (1, 128), 1)

    def owners_of(pair):
        b, h = pair // heads, pair % heads
        named = [picks[b, h, c] for c in range(columns)]
        found = []
        for c in range(columns):
            fresh = named[c] >= 0
            for earlier in range(c):
                fresh = fresh & (named[c] != named[earlier])
            block = jnp.maximum(named[c], 0)
            found.append((jnp.where(fresh, block // blocks, -1), block % blocks * heads + h))
        return found

    def place(pair, carry):
        wanted, used, owner_at = carry
        for c, (owner, code) in enumerate(owners_of(pair)):
            of_owner = lane % slots // CAP == owner
            hit = of_owner & (lane % CAP == used)
            wanted = jnp.where(hit, jnp.where(lane < slots, code, pair), wanted)
            used = jnp.where(of_owner, used + 1, used)
            owner_at = jnp.where(lane == pair * columns + c, owner, owner_at)
        return wanted, used, owner_at

    none = jnp.zeros((1, 128), jnp.int32)
    wanted, _, owner_at = lax.fori_loop(0, pairs, place, (none, none, none - 1))
    asks[y] = wanted

    def rank(pair, earlier):
        for c, (owner, _) in enumerate(owners_of(pair)):
            earlier += jnp.where((owner_at == owner) & (lane > pair * columns + c), 1, 0)
        return earlier

    ranks = lax.fori_loop(0, pairs, rank, none)
    asks[ny] = jnp.where(owner_at >= 0, owner_at * CAP + ranks, -1)
    for p in range(pairs):
        fetch(0, p).wait()
    pl.semaphore_wait(barrier, ny - 1 + nz - 1 + 3)

    def start_queries():
        from_below(lambda row: query_copy(row).start())

    def start_ring():
        for way in (0, 1):
            key_copy(way, 0).start()
        for way in (0, 1):
            value_copy(way, 0).start()

    from_below(lambda row: ask_copy(row).start())

    @pl.when(leads & in_ring)
    def _():
        key_copy(0, 0).start()
        key_copy(1, 0).start()

    @pl.when(helps)
    def _():
        over(0, z, lambda at: row_ask_copy(at).start())

    for p in range(pairs):
        fetch(1, p).wait()

    @pl.when(leads)
    def _():
        start_queries()

    for p in range(pairs):
        fetch(2, p).wait()
        values_t[0][p] = v_tiles[p].T

    @pl.when(in_ring)
    def _():
        lend_copy(y).start()

    @pl.when(leads & in_ring)
    def _():
        value_copy(0, 0).start()
        value_copy(1, 0).start()

    def begin_guests():
        def begin(row):
            remote(guest(0, row), guest(0, row), lend_s.at[0], lend_r.at[row],
                   along_y(row)).wait_recv()
            for way in (0, 1):
                guest_copy(row, way, 0).start()

        over(0, last, begin)

    pl.when(leads & helps)(begin_guests)

    def own(p, carry):
        own_part[p], own_stat[p] = tile_partial(
            queries[y, p], keys[0][p], values_t[0][p], True)
        return carry

    lax.fori_loop(0, pairs, own, 0)

    def greenlight(sem):
        pl.semaphore_signal(sem, inc=1, device_id={"head": mate}, device_id_type=MESH)

    @pl.when(leads & helps)
    def _():
        greenlight(q_go)

    total[...] = jnp.zeros_like(total)
    w_copy.wait()

    @pl.when(follows)
    def _():
        pl.semaphore_wait(q_go, 1)
        start_queries()
        pl.semaphore_wait(ring_go, 1)
        pl.when(in_ring)(start_ring)
        pl.when(helps)(begin_guests)

    from_above(lambda row: remote(
        asks.at[row], asks.at[row], ask_s.at[row], ask_r.at[row], along_y(row)).wait_recv())

    @pl.when(helps)
    def _():
        over(z + 1, nz, lambda at: remote(
            asks.at[ny + 1 + at], asks.at[ny + 1 + at], row_ask_s.at[at], row_ask_r.at[at],
            along_z(at)).wait_recv())

    ask_copy_in = pltpu.make_async_copy(asks, asks_sm, local_sem.at[1])
    ask_copy_in.start()
    ask_copy_in.wait()

    def serve_row(row, at, n):
        for s in range(CAP):
            lane_of = (y * nz + at) * CAP + s
            code = asks_sm[row, 0, lane_of]
            pair = asks_sm[row, 0, slots + lane_of]
            i = (row * nz + at) * CAP + s
            part_buf[i], stat_buf[i] = tile_partial(
                queries[row, pair], keys[n][code], values_t[n][code], False)

            @pl.when(row > y)
            def _():
                part_copy(row, at, s).start()

    def serve(at, n):
        def one(i, carry):
            row = ny - 1 - i

            @pl.when((row > y) | ((row == y) & (at < z)))
            def _():
                serve_row(row, at, n)

            @pl.when(row > y)
            def _():
                stat_copy(row, at).start()

            return carry

        lax.fori_loop(0, ny, one, 0)

    def take_back(n):
        here = values_t[n].at[pl.ds(kept, LENT)]
        remote(here, here, back_s.at[0, n], back_r.at[n], along_y(last)).wait_recv()

    def serve_both(step):
        for way, at in ((0, (z + nz - step) % nz), (1, (z + step) % nz)):
            take_back(held[way][step])
            serve(at, held[way][step])

    @pl.when(in_ring)
    def _():
        for step in range(1, half):
            for copy_of, final in ((key_copy, (0, 1)), (value_copy, (1,))):
                for way in (0, 1):
                    copy_of(way, step - 1).wait_recv()
                    if step < half - 1 or way in final:
                        copy_of(way, step).start()
            if step == 1:
                @pl.when(leads)
                def _():
                    greenlight(q_go)

                from_above(lambda row: remote(
                    queries.at[row], queries.at[row], q_s.at[row], q_r.at[row],
                    along_y(row)).wait_recv())
                serve(z, 0)
            if step == half - 2:
                @pl.when(leads)
                def _():
                    greenlight(ring_go)

            if step > 1:
                serve_both(step - 1)
        serve_both(half - 1)

    @pl.when(helps)
    def _():
        def ask_slot(at):
            for s in range(CAP):
                lane_of = (y * nz + at) * CAP + s
                slot_queries[at * CAP + s] = queries[y, asks_sm[y, 0, slots + lane_of]]

        def ask_slots():
            over(0, z, ask_slot)
            over(0, z, lambda at: slot_query_copy(at).start())

        for step in range(1, half):
            def onward(row):
                for way in (0, 1):
                    guest_copy(row, way, step - 1).wait_recv()
                    guest_copy(row, way, step).start()
                    back_copy(row, held[way][step]).start()

            over(0, last, onward)
            if step == 1:
                pl.when(follows)(ask_slots)

        def finish(row):
            for way in (0, 1):
                guest_copy(row, way, half - 1).wait_recv()
            back_copy(row, nz - 1).start()

        over(0, last, finish)

        @pl.when(leads)
        def _():
            greenlight(ring_go)

        pl.when(leads)(ask_slots)

        def serve_slots(at):
            here = slot_queries.at[pl.ds(at * CAP, CAP)]
            remote(here, here, slot_q_s.at[at], slot_q_r.at[at], along_z(at)).wait_recv()
            for s in range(CAP):
                code = asks_sm[ny + 1 + at, 0, (y * nz + z) * CAP + s]
                i = (y * nz + at) * CAP + s
                part_buf[i], stat_buf[i] = tile_partial(
                    slot_queries[at * CAP + s], keys[0][code], values_t[0][code], False)
                row_part_copy(at, s).start()
            row_stat_copy(at).start()

        over(z + 1, nz, serve_slots)

    parts = 2 * blocks
    tiles_in = pairs // parts

    def unit(g, u):
        return gathered.at[g, pl.ds(u * tiles_in, tiles_in)]

    def hop(g, u, way, k):
        return remote(unit(g, u), unit(g, u), ring_s.at[way, k], ring_r.at[way, k],
                      {"head": (right, left)[way]})

    def pass_over(g, u, k):
        return remote(unit(g, u), unit(g, u), mate_s.at[k], mate_r.at[k], {"head": mate})

    def project(g, u):
        tiles = jnp.concatenate(
            [gathered[g, u * tiles_in + t] for t in range(tiles_in)], axis=1)
        depth = tiles_in * width
        at = pl.multiple_of(g * heads * width + u % 2 * depth, depth)
        rows_of = pl.ds(u // 2 * rows, rows)
        total[rows_of, :] += jnp.dot(
            tiles, w_ref[pl.ds(at, depth), :], preferred_element_type=jnp.float32)

    orders = ((0, 1, 2, 3), (2, 3, 0, 1))
    arrivals = [((left, right)[way], orders[way][k], way, k) for k in range(parts)
                for way in (0, 1)]
    arrivals += [(across, orders[way][k], way, parts + k) for k in (0, 1) for way in (0, 1)]
    flip = 1 - 2 * (head_at % 2)

    def project_mates():
        for u in (0, 2, 1, 3):
            pass_over(mate, u, u).wait_recv()
            project(mate, u)
        for n, (g, u, _, _) in enumerate(arrivals):
            pass_over(g + flip, u, parts + n).wait_recv()
            project(g + flip, u)

    @pl.when(in_ring)
    def _():
        key_copy(0, half - 1).wait_recv()
        key_copy(1, half - 1).wait_recv()
        take_back(nz - 1)
        value_copy(1, half - 1).wait_recv()
        serve((z + half) % nz, nz - 1)

    def collect(row):
        def one(n, carry):
            here = part_buf.at[row * nz * CAP + n]
            remote(here, here, part_s.at[row, n], part_r.at[row, n], along_y(row)).wait_recv()
            return carry

        def other(at, carry):
            here = stat_buf.at[pl.ds((row * nz + at) * CAP, CAP)]
            remote(here, here, stat_s.at[row, at], stat_r.at[row, at], along_y(row)).wait_recv()
            return carry

        lax.fori_loop(0, nz * CAP, one, 0)
        lax.fori_loop(0, nz, other, 0)

    pl.when(follows)(project_mates)
    from_below(collect)

    @pl.when(helps)
    def _():
        def collect_slots(at):
            for s in range(CAP):
                here = part_buf.at[(y * nz + at) * CAP + s]
                n = at * CAP + s
                remote(here, here, part_s.at[y, n], part_r.at[y, n], along_z(at)).wait_recv()
            here = stat_buf.at[pl.ds((y * nz + at) * CAP, CAP)]
            remote(here, here, stat_s.at[y, at], stat_r.at[y, at], along_z(at)).wait_recv()

        over(0, z, collect_slots)

    def merge(p, carry):
        stats = [own_stat[p]]
        used = [None]
        slots = [None]
        for c in range(columns):
            slot = asks_sm[ny, 0, p * columns + c]
            used.append(slot >= 0)
            slots.append(jnp.maximum(slot, 0))
            stats.append(stat_buf[slots[-1]])
        tops = [stats[0][:1]] + [
            jnp.where(used[i], stats[i][:1], -1e30) for i in range(1, columns + 1)]
        largest = functools.reduce(jnp.maximum, tops)
        factor = jnp.exp2(tops[0] - largest)
        numer = factor * own_part[p].astype(jnp.float32)
        denom = factor * stats[0][1:]
        for i in range(1, columns + 1):
            factor = jnp.exp2(tops[i] - largest)
            numer += jnp.where(used[i], factor * part_buf[slots[i]].astype(jnp.float32), 0.0)
            denom += jnp.where(used[i], factor * stats[i][1:], 0.0)
        gathered[head_at, p] = (numer * (1.0 / denom)).astype(jnp.bfloat16).T
        return carry

    sends = []

    def start(copy):
        copy.start()
        sends.append(copy)

    for u, way in ((0, 0), (2, 1), (1, 0), (3, 1)):
        lax.fori_loop(u * tiles_in, (u + 1) * tiles_in, merge, 0)
        start(hop(head_at, u, way, u % 2))
        start(pass_over(head_at, u, u))
    for u, way in ((2, 0), (0, 1), (3, 0), (1, 1)):
        start(hop(head_at, u, way, 2 + u % 2))
    for u in range(parts):
        project(head_at, u)
    for n, (g, u, way, k) in enumerate(arrivals):
        hop(g, u, way, k).wait_recv()
        if k < 2:
            start(hop(g, u, way, parts + k))
        start(pass_over(g, u, parts + n))
        project(g, u)
    pl.when(leads)(project_mates)
    out_ref[...] = total[...].astype(out_ref.dtype)

    def drain_below(row):
        ask_copy(row).wait_send()
        query_copy(row).wait_send()

    def drain_above(row):
        def one(at, carry):
            for s in range(CAP):
                part_copy(row, at, s).wait_send()
            stat_copy(row, at).wait_send()
            return carry

        lax.fori_loop(0, nz, one, 0)

    from_below(drain_below)
    from_above(drain_above)

    @pl.when(in_ring)
    def _():
        lend_copy(y).wait_send()
        for way in (0, 1):
            for step in range(half):
                key_copy(way, step).wait_send()
                if step < half - 1 or way == 1:
                    value_copy(way, step).wait_send()

    @pl.when(helps)
    def _():
        def drain_asks(at):
            row_ask_copy(at).wait_send()
            slot_query_copy(at).wait_send()

        def drain_parts(at):
            for s in range(CAP):
                row_part_copy(at, s).wait_send()
            row_stat_copy(at).wait_send()

        def drain_guests(row):
            for way in (0, 1):
                for step in range(half):
                    guest_copy(row, way, step).wait_send()
            for n in range(1, nz):
                back_copy(row, n).wait_send()

        over(0, z, drain_asks)
        over(z + 1, nz, drain_parts)
        over(0, last, drain_guests)

    for copy in sends:
        copy.wait_send()


def attend_and_project(picks, query_rows, key_rows, value_rows, out_weight, rings, groups):
    ny, nz = rings
    blocks, heads, _ = picks.shape
    tok_rows, feature = query_rows.shape
    width, rows, pairs = feature // heads, tok_rows // blocks, blocks * heads
    slots = ny * nz * CAP
    hbm = pl.BlockSpec(memory_space=pl.ANY)
    dma = pltpu.SemaphoreType.DMA
    bf16, f32, i32 = jnp.bfloat16, jnp.float32, jnp.int32
    return pl.pallas_call(
        functools.partial(main_kernel, rings),
        out_shape=jax.ShapeDtypeStruct((tok_rows, out_weight.shape[1]), bf16),
        in_specs=[pl.BlockSpec(memory_space=pltpu.SMEM), hbm, hbm, hbm, hbm],
        out_specs=pl.BlockSpec(memory_space=pltpu.VMEM),
        scratch_shapes=[
            pltpu.VMEM((ny, pairs, rows, width), bf16),
            pltpu.VMEM((pairs, rows, width), bf16),
            pltpu.VMEM((pairs, width, rows), bf16),
            pltpu.VMEM((pairs, 2, rows), f32),
            pltpu.VMEM((ny + 1 + nz, 1, 128), i32),
            pltpu.SMEM((ny + 1 + nz, 1, 128), i32),
            pltpu.VMEM((slots, width, rows), bf16),
            pltpu.VMEM((slots, 2, rows), f32),
            pltpu.VMEM((groups, pairs, rows, width), bf16),
            pltpu.VMEM((tok_rows, out_weight.shape[1]), f32),
            pltpu.VMEM(out_weight.shape, bf16),
        ]
        + [dma((ny,)) for _ in range(4)]
        + [dma((ny, nz * CAP)) for _ in range(2)]
        + [dma((ny, nz)) for _ in range(2)]
        + [dma((2, nz // 2)) for _ in range(4)]
        + [dma((2,)), dma((3, pairs)), dma((2, 6)), dma((2, 6)), dma((16,)), dma((16,))]
        + [pltpu.SemaphoreType.REGULAR] * 2
        + [pltpu.VMEM(((ny - 1) * LENT, width, rows), bf16),
           pltpu.VMEM((nz * CAP, rows, width), bf16)]
        + [dma((nz,)) for _ in range(4)]
        + [dma((1,)), dma((ny - 1,))]
        + [dma((ny - 1, 2, nz // 2)) for _ in range(2)]
        + [dma((ny - 1, nz)), dma((nz,))]
        + [pltpu.VMEM((pairs, rows, width), bf16) for _ in range(nz)]
        + [pltpu.VMEM((pairs, width, rows), bf16) for _ in range(nz)],
        compiler_params=pltpu.CompilerParams(
            collective_id=0, has_side_effects=True, vmem_limit_bytes=60 * 1024 * 1024),
    )(picks, query_rows, key_rows, value_rows, out_weight)


def solution(mesh):
    rings, groups = RINGS[mesh.shape["seq"]], mesh.shape["head"]

    def body(query_rows, key_rows, value_rows, block_picks, out_weight):
        return attend_and_project(
            block_picks, query_rows, key_rows, value_rows, out_weight, rings, groups)

    return jax.shard_map(
        body,
        mesh=mesh,
        in_specs=(
            P("seq", "head"),
            P("seq", "head"),
            P("seq", "head"),
            P("seq", "head", None),
            P(None, "head"),
        ),
        out_specs=P("seq", "head"),
        check_vma=False,
    )
```
